8 devices in a mesh: rep: 1 (over z), dp: 8 (over x, y, core).
Axes of the slice: x: 2, y: 2, z: 1, core: 2. Of those that a mesh axis runs over, the one named last changes fastest.
Arguments:
- x: bfloat16 [8, 2048, 1024], P(('rep', 'dp'))
- dy: bfloat16 [8, 2048, 1024], P(('rep', 'dp'))
- wq: bfloat16 [2, 1024, 1024], replicated
- wk: bfloat16 [2, 1024, 1024], replicated
- wv: bfloat16 [2, 1024, 1024], replicated
- wo: bfloat16 [2, 1024, 1024], replicated
- w_gate: bfloat16 [2, 1024, 4096], replicated
- w_up: bfloat16 [2, 1024, 4096], replicated
- w_down: bfloat16 [2, 4096, 1024], replicated
- m_wq: float32 [2, 1024, 1024], replicated
- m_wk: float32 [2, 1024, 1024], replicated
- m_wv: float32 [2, 1024, 1024], replicated
- m_wo: float32 [2, 1024, 1024], replicated
- m_w_gate: float32 [2, 1024, 4096], replicated
- m_w_up: float32 [2, 1024, 4096], replicated
- m_w_down: float32 [2, 4096, 1024], replicated
- v_wq: float32 [2, 1024, 1024], replicated
- v_wk: float32 [2, 1024, 1024], replicated
- v_wv: float32 [2, 1024, 1024], replicated
- v_wo: float32 [2, 1024, 1024], replicated
- v_w_gate: float32 [2, 1024, 4096], replicated
- v_w_up: float32 [2, 1024, 4096], replicated
- v_w_down: float32 [2, 4096, 1024], replicated
Outputs:
- output 1: bfloat16 [2, 1024, 1024], P('rep')
- output 2: bfloat16 [2, 1024, 1024], P('rep')
- output 3: bfloat16 [2, 1024, 1024], P('rep')
- output 4: bfloat16 [2, 1024, 1024], P('rep')
- output 5: bfloat16 [2, 1024, 4096], P('rep')
- output 6: bfloat16 [2, 1024, 4096], P('rep')
- output 7: bfloat16 [2, 4096, 1024], P('rep')
- output 8: float32 [2, 1024, 1024], P('rep')
- output 9: float32 [2, 1024, 1024], P('rep')
- output 10: float32 [2, 1024, 1024], P('rep')
- output 11: float32 [2, 1024, 1024], P('rep')
- output 12: float32 [2, 1024, 4096], P('rep')
- output 13: float32 [2, 1024, 4096], P('rep')
- output 14: float32 [2, 4096, 1024], P('rep')
- output 15: float32 [2, 1024, 1024], P('rep')
- output 16: float32 [2, 1024, 1024], P('rep')
- output 17: float32 [2, 1024, 1024], P('rep')
- output 18: float32 [2, 1024, 1024], P('rep')
- output 19: float32 [2, 1024, 4096], P('rep')
- output 20: float32 [2, 1024, 4096], P('rep')
- output 21: float32 [2, 4096, 1024], P('rep')
All inputs are finite; a program needn't handle non-finite values.
Results may differ from the reference program's by a relative error of at most 0.024.
Values are sent between devices in bfloat16 or wider.
A program may use at most 3 GiB of HBM per device.

```python
import jax
import jax.numpy as jnp
from jax import lax

SEQUENCES = 8
TOKENS = 2048
D = 1024
HEADS = 4
KV_HEADS = 4
HEAD = 256
FF = 4096
LAYERS = 2
THETA = 10000
NAMES = ("wq", "wk", "wv", "wo", "w_gate", "w_up", "w_down")
SHAPES = {
    "wq": (LAYERS, D, HEADS * HEAD),
    "wk": (LAYERS, D, KV_HEADS * HEAD),
    "wv": (LAYERS, D, KV_HEADS * HEAD),
    "wo": (LAYERS, HEADS * HEAD, D),
    "w_gate": (LAYERS, D, FF),
    "w_up": (LAYERS, D, FF),
    "w_down": (LAYERS, FF, D),
}


def bump(key, n, height):
    away = (jnp.arange(n, dtype=jnp.int32) - jax.random.randint(key, (), 0, n, jnp.int32)) % n
    return jnp.where(away < n // 8, height, 1.0)


def together(key, own, strength):
    shared = jax.random.normal(key, own.shape[1:], jnp.float32)
    return (own + strength * shared) * lax.rsqrt(1 + strength * strength)


def setup_inputs(seed: int = 0, part: int = 0) -> dict:
    kx, kdy, ka, kb, kz, kf, kh, kl, *keys = jax.random.split(jax.random.key(seed), 8 + 3 * len(NAMES))
    kx, kdy, ka, kb = (jax.random.fold_in(k, part) for k in (kx, kdy, ka, kb))
    kw, km, kv = (keys[i::3] for i in range(3))
    shape = (SEQUENCES, TOKENS, D)
    much_x, much_dy = jax.random.uniform(kz, (2,), jnp.float32, 0.0, 1.0)
    loud = 2.0 ** jax.random.uniform(jax.random.fold_in(kz, 1), (), jnp.float32, -1.0, 2.0)
    layers = 2.0 ** jax.random.uniform(kl, (LAYERS, 1, 1), jnp.float32, -1.0, 1.0)
    times = {"wq": 1.0, "wk": 1.0, "wv": 2.0, "wo": layers, "w_gate": 1.0, "w_up": bump(kh, FF, 4.0), "w_down": layers}
    x = together(ka, jax.random.normal(kx, shape, jnp.float32), much_x) * bump(kf, D, 4.0)
    dy = together(kb, jax.random.normal(kdy, shape, jnp.float32), much_dy)
    drawn = {"x": x.astype(jnp.bfloat16), "dy": (loud * dy * (SEQUENCES * TOKENS) ** -0.5).astype(jnp.bfloat16)}
    for key, name in zip(kw, NAMES, strict=True):
        drawn[name] = (jax.random.normal(key, SHAPES[name], jnp.float32) * SHAPES[name][1] ** -0.5 * times[name]).astype(jnp.bfloat16)
    for key, name in zip(km, NAMES, strict=True):
        drawn[f"m_{name}"] = 0.1 * jax.random.normal(key, SHAPES[name], jnp.float32)
    for key, name in zip(kv, NAMES, strict=True):
        drawn[f"v_{name}"] = jax.random.uniform(key, SHAPES[name], jnp.float32, 0.02, 0.06)
    return drawn


def matmul(a, w):
    return jnp.dot(a, w, preferred_element_type=jnp.float32).astype(jnp.bfloat16)


def normed(h):
    wide = h.astype(jnp.float32)
    scale = lax.rsqrt(jnp.mean(wide**2, -1, keepdims=True) + 1e-6)
    return (wide * scale).astype(jnp.bfloat16)


def turned(t, theta):
    half = t.shape[-1] // 2
    angle = jnp.arange(t.shape[0], dtype=jnp.float32)[:, None] * theta ** (-jnp.arange(half, dtype=jnp.float32) / half)
    cos, sin = jnp.cos(angle)[:, None], jnp.sin(angle)[:, None]
    a, b = t[..., :half].astype(jnp.float32), t[..., half:].astype(jnp.float32)
    return jnp.concatenate([a * cos - b * sin, b * cos + a * sin], -1).astype(jnp.bfloat16)


def seen_by(q, k, v):
    tokens, kv = q.shape[0], k.shape[1]
    q = q.reshape(tokens, kv, -1, q.shape[-1])
    scores = jnp.einsum("tgsd,ugd->gstu", q.astype(jnp.float32), k.astype(jnp.float32)) * q.shape[-1] ** -0.5
    place = jnp.arange(tokens)
    weights = jax.nn.softmax(jnp.where(place[:, None] >= place, scores, -jnp.inf), -1).astype(jnp.bfloat16)
    return jnp.einsum("gstu,ugd->tgsd", weights.astype(jnp.float32), v.astype(jnp.float32)).astype(jnp.bfloat16).reshape(tokens, -1)


def layer(h, w):
    a = normed(h)
    q, k = (turned(matmul(a, w[name]).reshape(h.shape[0], -1, HEAD), THETA) for name in ("wq", "wk"))
    h = h + matmul(seen_by(q, k, matmul(a, w["wv"]).reshape(h.shape[0], -1, HEAD)), w["wo"])
    b = normed(h)
    gate = jnp.dot(b, w["w_gate"], preferred_element_type=jnp.float32)
    up = jnp.dot(b, w["w_up"], preferred_element_type=jnp.float32)
    return h + matmul((jax.nn.silu(gate) * up).astype(jnp.bfloat16), w["w_down"])


def adamw(w, m, v, g):
    m = 0.9 * m + 0.1 * g
    v = 0.95 * v + 0.05 * g * g
    step = m * lax.rsqrt(v + 1e-8) + 0.1 * w
    return (w - 0.02 * step).astype(jnp.bfloat16), m, v


def clipped(gradients, sum_of_squares, count):
    factor = jnp.minimum(1.0, 0.5 * lax.rsqrt(sum_of_squares / count + 1e-30))
    return [g * factor for g in gradients]


def stack(weights, h):
    return lax.scan(lambda h, w: (layer(h, w), None), h, weights)[0]


def reference(x, dy, wq, wk, wv, wo, w_gate, w_up, w_down, m_wq, m_wk, m_wv, m_wo, m_w_gate, m_w_up, m_w_down, v_wq, v_wk, v_wv, v_wo, v_w_gate, v_w_up, v_w_down):
    weights = dict(zip(NAMES, (wq, wk, wv, wo, w_gate, w_up, w_down), strict=True))

    def take(so_far, sequence):
        h, by_y = sequence
        _, back = jax.vjp(stack, weights, h)
        by_weights, by_h = back(by_y)
        return jax.tree.map(lambda total, term: total + term.astype(jnp.float32), so_far, by_weights), by_h

    none_yet = {name: jnp.zeros(w.shape, jnp.float32) for name, w in weights.items()}
    by_weights, by_x = lax.scan(take, none_yet, (x, dy))
    gradients = [by_weights[name].astype(jnp.bfloat16).astype(jnp.float32) for name in NAMES]
    gradients = clipped(gradients, sum(jnp.sum(g * g) for g in gradients), sum(g.size for g in gradients))
    first = (m_wq, m_wk, m_wv, m_wo, m_w_gate, m_w_up, m_w_down)
    second = (v_wq, v_wk, v_wv, v_wo, v_w_gate, v_w_up, v_w_down)
    new = [adamw(weights[name].astype(jnp.float32), m, v, g) for name, m, v, g in zip(NAMES, first, second, gradients, strict=True)]
    return tuple(one[which] for which in range(3) for one in new)
```

```python
import functools

import jax
import jax.numpy as jnp
from jax import lax
from jax.experimental import pallas as pl
from jax.experimental.pallas import tpu as pltpu
from jax.sharding import PartitionSpec as P

NAMES = ("wq", "wk", "wv", "wo", "w_gate", "w_up", "w_down")
HEAD = 256
THETA = 10000
EPS = 1e-6
LOG2E = 1.4426950408889634
HIDDEN = -2e30
f32, bf16 = jnp.float32, jnp.bfloat16
VMEM = 63 * 2**20
ONE = pl.Buffered(1)


def dot(a, b, ca=1, cb=0):
    return lax.dot_general(a, b, (((ca,), (cb,)), ((), ())), preferred_element_type=f32)


def rows_of(i, n):
    return pl.ds(pl.multiple_of(i * n, n), n)


def inv_rms(h):
    return lax.rsqrt(jnp.mean(h * h, -1, keepdims=True) + EPS)


def norm_back(h, by_out):
    scale = inv_rms(h)
    return scale * (by_out - h * (scale * scale * jnp.mean(by_out * h, -1, keepdims=True)))


def params(**more):
    return pltpu.CompilerParams(dimension_semantics=("arbitrary",), vmem_limit_bytes=VMEM, **more)


def _qkv(x_ref, wq_ref, wk_ref, wv_ref, cos_ref, sin_ref, q_ref, k_ref, v_ref):
    x = x_ref[...].astype(f32)
    a = (x * inv_rms(x)).astype(bf16)
    cos, sin = cos_ref[...], sin_ref[...]
    for w_ref, o_ref in ((wq_ref, q_ref), (wk_ref, k_ref)):
        t = dot(a, w_ref[...]).astype(bf16).astype(f32)
        half = HEAD // 2
        for h in range(t.shape[1] // HEAD):
            p, r = t[:, h * HEAD : h * HEAD + half], t[:, h * HEAD + half : (h + 1) * HEAD]
            o_ref[:, h * HEAD : h * HEAD + half] = (p * cos - r * sin).astype(bf16)
            o_ref[:, h * HEAD + half : (h + 1) * HEAD] = (r * cos + p * sin).astype(bf16)
    v_ref[...] = dot(a, wv_ref[...]).astype(bf16)


def qkv(x, wq, wk, wv, cos, sin, layer, tm=512):
    t, d = x.shape
    row = pl.BlockSpec((tm, d), lambda i: (i, 0))
    w = pl.BlockSpec((None, d, d), lambda i: (layer, 0, 0), pipeline_mode=ONE)
    tab = pl.BlockSpec((tm, HEAD // 2), lambda i: (i, 0))
    return pl.pallas_call(
        _qkv, grid=(t // tm,), in_specs=[row, w, w, w, tab, tab], out_specs=[row] * 3,
        out_shape=[jax.ShapeDtypeStruct((t, d), bf16)] * 3, compiler_params=params(), name="qkv",
    )(x, wq, wk, wv, cos, sin)


def _attn(q_ref, k_ref, v_ref, x_ref, wo_ref, o_ref, lse_ref, h_ref, o_s, s_s, p_s, *, blk, scale):
    head = pl.program_id(0)
    t = q_ref.shape[0]
    e = scale * LOG2E
    vt = jnp.concatenate([v_ref[...].T, jnp.ones((16, t), bf16)], axis=0)
    for i in range(t // blk):
        here = pl.ds(i * blk, blk)
        q = q_ref[here, :]
        top = None
        for j in range(i + 1):
            s = dot(k_ref[j * blk : (j + 1) * blk, :], q, 1, 1)
            if i == j:
                gap = lax.broadcasted_iota(jnp.int32, (blk, blk), 1) - lax.broadcasted_iota(jnp.int32, (blk, blk), 0)
                s = jnp.where(gap >= 0, s, HIDDEN)
            s_s[j * blk : (j + 1) * blk, :] = s
            m = s.max(axis=0, keepdims=True)
            top = m if top is None else jnp.maximum(top, m)
        for j in range(i + 1):
            p_s[j * blk : (j + 1) * blk, :] = jnp.exp2((s_s[j * blk : (j + 1) * blk, :] - top) * e).astype(bf16)
        n = (i + 1) * blk
        mix = dot(vt[:, :n], p_s[:n, :])
        total = mix[HEAD : HEAD + 1, :]
        o = (mix[:HEAD, :] * (1 / total)).T.astype(bf16)
        o_ref[here, :] = o
        o_s[head, here, :] = o
        lse_ref[0, :, here] = top * scale + jnp.log(total)

    @pl.when(head == pl.num_programs(0) - 1)
    def _():
        def row(r, _):
            here = rows_of(r, 512)
            o = jnp.concatenate([o_s[n, here, :] for n in range(o_s.shape[0])], axis=1)
            h_ref[here, :] = (x_ref[here, :].astype(f32) + dot(o, wo_ref[...]).astype(bf16).astype(f32)).astype(bf16)
            return _

        lax.fori_loop(0, t // 512, row, None)


def attn(q, k, v, x, wo, layer, blk=512):
    t, d = x.shape
    heads = d // HEAD
    one = pl.BlockSpec((t, HEAD), lambda h: (0, h))
    full = pl.BlockSpec((t, d), lambda h: (0, 0), pipeline_mode=ONE)
    return pl.pallas_call(
        functools.partial(_attn, blk=blk, scale=HEAD**-0.5), grid=(heads,),
        in_specs=[one, one, one, full, pl.BlockSpec((None, d, d), lambda h: (layer, 0, 0), pipeline_mode=ONE)],
        out_specs=[one, pl.BlockSpec((1, 1, t), lambda h: (h, 0, 0)), full],
        out_shape=[jax.ShapeDtypeStruct((t, d), bf16), jax.ShapeDtypeStruct((heads, 1, t), f32), jax.ShapeDtypeStruct((t, d), bf16)],
        scratch_shapes=[pltpu.VMEM((heads, t, HEAD), bf16), pltpu.VMEM((t, blk), f32), pltpu.VMEM((t, blk), bf16)],
        compiler_params=params(), name="attn",
    )(q, k, v, x, wo)


def _mlp(h_ref, wg_ref, wu_ref, wd_ref, y_ref, b_s, acc_s, *, tm):
    j = pl.program_id(0)
    t = h_ref.shape[0]

    @pl.when(j == 0)
    def _():
        def pre(r, _):
            here = rows_of(r, 256)
            h = h_ref[here, :].astype(f32)
            b_s[here, :] = (h * inv_rms(h)).astype(bf16)
            acc_s[here, :] = jnp.zeros((256, acc_s.shape[1]), f32)
            return _

        lax.fori_loop(0, t // 256, pre, None)

    def row(r, _):
        here = rows_of(r, tm)
        b = b_s[here, :]
        gate, up = dot(b, wg_ref[...]), dot(b, wu_ref[...])
        act = (gate * (1.0 / (1.0 + jnp.exp(-gate))) * up).astype(bf16)
        acc_s[here, :] += dot(act, wd_ref[...])
        return _

    lax.fori_loop(0, t // tm, row, None)

    @pl.when(j == pl.num_programs(0) - 1)
    def _():
        def post(r, _):
            here = rows_of(r, 256)
            y_ref[here, :] = (h_ref[here, :].astype(f32) + acc_s[here, :].astype(bf16).astype(f32)).astype(bf16)
            return _

        lax.fori_loop(0, t // 256, post, None)


def mlp(h, wg, wu, wd, layer, tf=512, tm=512):
    t, d = h.shape
    ff = wg.shape[2]
    full = pl.BlockSpec((t, d), lambda j: (0, 0), pipeline_mode=ONE)
    cols = pl.BlockSpec((None, d, tf), lambda j: (layer, 0, j))
    return pl.pallas_call(
        functools.partial(_mlp, tm=tm), grid=(ff // tf,),
        in_specs=[full, cols, cols, pl.BlockSpec((None, tf, d), lambda j: (layer, j, 0))], out_specs=full,
        out_shape=jax.ShapeDtypeStruct((t, d), bf16),
        scratch_shapes=[pltpu.VMEM((t, d), bf16), pltpu.VMEM((t, d), f32)],
        compiler_params=params(), name="mlp",
    )(h, wg, wu, wd)


def _mlp_back(h_ref, dy_ref, wg_ref, wu_ref, wd_ref, dwg_ref, dwu_ref, dwd_ref, dh_ref, b_s, bt_s, acc_s, at_s, dg_s, du_s, *, tm, dm):
    j = pl.program_id(0)
    t, d = h_ref.shape
    tf = wg_ref.shape[1]

    @pl.when(j == 0)
    def _():
        def pre(r, _):
            here = rows_of(r, 256)
            h = h_ref[here, :].astype(f32)
            b = (h * inv_rms(h)).astype(bf16)
            b_s[here, :] = b
            bt_s[:, here] = b.T
            acc_s[here, :] = jnp.zeros((256, d), f32)
            return _

        lax.fori_loop(0, t // 256, pre, None)

    def row(r, _):
        here = rows_of(r, tm)
        b = b_s[here, :]
        gate, up = dot(b, wg_ref[...]), dot(b, wu_ref[...])
        da = dot(dy_ref[here, :], wd_ref[...], 1, 1).astype(bf16).astype(f32)
        s = 1.0 / (1.0 + jnp.exp(-gate))
        silu = gate * s
        at_s[:, here] = (silu * up).astype(bf16).T
        du = (da * silu).astype(bf16)
        dg = (da * up * (s * (1.0 + gate * (1.0 - s)))).astype(bf16)
        du_s[here, :] = du
        dg_s[here, :] = dg
        acc_s[here, :] += dot(dg, wg_ref[...], 1, 1) + dot(du, wu_ref[...], 1, 1)
        return _

    lax.fori_loop(0, t // tm, row, None)

    def col(r, _):
        here = rows_of(r, dm)
        bt = bt_s[here, :]
        dwg_ref[here, :] = dot(bt, dg_s[...]).astype(bf16)
        dwu_ref[here, :] = dot(bt, du_s[...]).astype(bf16)
        return _

    lax.fori_loop(0, d // dm, col, None)
    dwd_ref[...] = dot(at_s[...], dy_ref[...]).astype(bf16)

    @pl.when(j == pl.num_programs(0) - 1)
    def _():
        def post(r, _):
            here = rows_of(r, 256)
            by_b = acc_s[here, :].astype(bf16).astype(f32)
            dh_ref[here, :] = (dy_ref[here, :].astype(f32) + norm_back(h_ref[here, :].astype(f32), by_b)).astype(bf16)
            return _

        lax.fori_loop(0, t // 256, post, None)


def mlp_back(h, dy, wg, wu, wd, layer, tf=512, tm=512, dm=512):
    t, d = h.shape
    ff = wg.shape[2]
    full = pl.BlockSpec((t, d), lambda j: (0, 0), pipeline_mode=ONE)
    cols = pl.BlockSpec((None, d, tf), lambda j: (layer, 0, j))
    grad = pl.BlockSpec((d, tf), lambda j: (0, j))
    return pl.pallas_call(
        functools.partial(_mlp_back, tm=tm, dm=dm), grid=(ff // tf,),
        in_specs=[full, full, cols, cols, pl.BlockSpec((None, tf, d), lambda j: (layer, j, 0))],
        out_specs=[grad, grad, pl.BlockSpec((tf, d), lambda j: (j, 0)), full],
        out_shape=[jax.ShapeDtypeStruct((d, ff), bf16)] * 2 + [jax.ShapeDtypeStruct((ff, d), bf16), jax.ShapeDtypeStruct((t, d), bf16)],
        scratch_shapes=[pltpu.VMEM((t, d), bf16), pltpu.VMEM((d, t), bf16), pltpu.VMEM((t, d), f32),
                        pltpu.VMEM((tf, t), bf16), pltpu.VMEM((t, tf), bf16), pltpu.VMEM((t, tf), bf16)],
        compiler_params=params(), name="mlp_back",
    )(h, dy, wg, wu, wd)


def _attn_back(x_ref, dh_ref, q_ref, k_ref, v_ref, o_ref, lse_ref, wq_ref, wk_ref, wv_ref, wo_ref, cos_ref, sin_ref,
               dwq_ref, dwk_ref, dwv_ref, dwo_ref, dx_ref, at_s, acc_s, do_s, delta_s, p_s, ds_s, dqt_s, dk_s, dv_s, g_s,
               *, blk, scale, inner):
    head = pl.program_id(0)
    t, d = x_ref.shape
    n = t // blk
    e = scale * LOG2E

    @pl.when(head == 0)
    def _():
        def pre(r, _):
            here = rows_of(r, 256)
            h = x_ref[here, :].astype(f32)
            at_s[:, here] = (h * inv_rms(h)).astype(bf16).T
            if inner:
                acc_s[here, :] = jnp.zeros((256, d), f32)
            return _

        lax.fori_loop(0, t // 256, pre, None)

    for i in range(n):
        here = pl.ds(i * blk, blk)
        do = dot(dh_ref[here, :], wo_ref[...], 1, 1).astype(bf16)
        do_s[here, :] = do
        delta = jnp.sum(do.astype(f32) * o_ref[here, :].astype(f32), -1, keepdims=True)
        delta_s[:, here] = jnp.broadcast_to(delta, (blk, 128)).T[:8, :]
    dwo_ref[...] = dot(o_ref[...].T, dh_ref[...]).astype(bf16)

    dqt_s[...] = jnp.zeros_like(dqt_s)
    for j in range(n):
        kj, vj = k_ref[j * blk : (j + 1) * blk, :], v_ref[j * blk : (j + 1) * blk, :]
        for i in range(j, n):
            cols = pl.ds(i * blk, blk)
            s = dot(kj, q_ref[cols, :], 1, 1)
            dp = dot(vj, do_s[cols, :], 1, 1)
            p = jnp.exp2(s * e - lse_ref[0, :, cols] * LOG2E)
            if i == j:
                gap = lax.broadcasted_iota(jnp.int32, (blk, blk), 1) - lax.broadcasted_iota(jnp.int32, (blk, blk), 0)
                p = jnp.where(gap >= 0, p, 0.0)
            p_s[:, cols] = p.astype(bf16)
            ds_s[:, cols] = (p * (dp - delta_s[0:1, cols])).astype(bf16)
        seen = slice(j * blk, t)
        dv_s[j * blk : (j + 1) * blk, :] = dot(p_s[:, seen], do_s[seen, :]).astype(bf16)
        dk_s[j * blk : (j + 1) * blk, :] = dot(ds_s[:, seen], q_ref[seen, :])
        dqt_s[:, seen] += dot(kj.T, ds_s[:, seen])

    half = HEAD // 2
    for i in range(n):
        here = pl.ds(i * blk, blk)
        cos, sin = cos_ref[here, :], sin_ref[here, :]
        for which, g in ((0, dqt_s[:, here].T), (1, dk_s[here, :])):
            g = (g * scale).astype(bf16).astype(f32)
            a, b = g[:, :half], g[:, half:]
            g_s[here, which * HEAD : which * HEAD + half] = (a * cos + b * sin).astype(bf16)
            g_s[here, which * HEAD + half : (which + 1) * HEAD] = (b * cos - a * sin).astype(bf16)

    dwq_ref[...] = dot(at_s[...], g_s[:, :HEAD]).astype(bf16)
    dwk_ref[...] = dot(at_s[...], g_s[:, HEAD:]).astype(bf16)
    dwv_ref[...] = dot(at_s[...], dv_s[...]).astype(bf16)
    if inner:
        for i in range(n):
            here = pl.ds(i * blk, blk)
            acc_s[here, :] += (dot(g_s[here, :HEAD], wq_ref[...], 1, 1) + dot(g_s[here, HEAD:], wk_ref[...], 1, 1)
                               + dot(dv_s[here, :], wv_ref[...], 1, 1))

        @pl.when(head == pl.num_programs(0) - 1)
        def _():
            def post(r, _):
                here = rows_of(r, 256)
                by_a = acc_s[here, :].astype(bf16).astype(f32)
                dx_ref[here, :] = (dh_ref[here, :].astype(f32) + norm_back(x_ref[here, :].astype(f32), by_a)).astype(bf16)
                return _

            lax.fori_loop(0, t // 256, post, None)


def attn_back(x, dh, q, k, v, o, lse, wq, wk, wv, wo, cos, sin, layer, inner, blk=512):
    t, d = x.shape
    heads = d // HEAD
    full = pl.BlockSpec((t, d), lambda h: (0, 0), pipeline_mode=ONE)
    one = pl.BlockSpec((t, HEAD), lambda h: (0, h))
    cols = pl.BlockSpec((None, d, HEAD), lambda h: (layer, 0, h))
    tab = pl.BlockSpec((t, HEAD // 2), lambda h: (0, 0), pipeline_mode=ONE)
    grad = pl.BlockSpec((d, HEAD), lambda h: (0, h))
    dx = jax.ShapeDtypeStruct((t, d), bf16) if inner else jax.ShapeDtypeStruct((8, 128), bf16)
    return pl.pallas_call(
        functools.partial(_attn_back, blk=blk, scale=HEAD**-0.5, inner=inner), grid=(heads,),
        in_specs=[full, full, one, one, one, one, pl.BlockSpec((1, 1, t), lambda h: (h, 0, 0)), cols, cols, cols,
                  pl.BlockSpec((None, HEAD, d), lambda h: (layer, h, 0)), tab, tab],
        out_specs=[grad, grad, grad, pl.BlockSpec((HEAD, d), lambda h: (h, 0)), full if inner else pl.BlockSpec((8, 128), lambda h: (0, 0))],
        out_shape=[jax.ShapeDtypeStruct((d, d), bf16)] * 4 + [dx],
        scratch_shapes=[pltpu.VMEM((d, t), bf16), pltpu.VMEM((t, d) if inner else (8, 128), f32), pltpu.VMEM((t, HEAD), bf16),
                        pltpu.VMEM((8, t), f32), pltpu.VMEM((blk, t), bf16), pltpu.VMEM((blk, t), bf16), pltpu.VMEM((HEAD, t), f32),
                        pltpu.VMEM((t, HEAD), f32), pltpu.VMEM((t, HEAD), bf16), pltpu.VMEM((t, 2 * HEAD), bf16)],
        compiler_params=params(), name="attn_back",
    )(x, dh, q, k, v, o, lse, wq, wk, wv, wo, cos, sin)


def tables(t):
    half = HEAD // 2
    angle = jnp.arange(t, dtype=f32)[:, None] * THETA ** (-jnp.arange(half, dtype=f32) / half)
    return jnp.cos(angle), jnp.sin(angle)


def adamw(w, m, v, g):
    m = 0.9 * m + 0.1 * g
    v = 0.95 * v + 0.05 * g * g
    step = m * lax.rsqrt(v + 1e-8) + 0.1 * w
    return (w - 0.02 * step).astype(bf16), m, v


def clipped(gradients, sum_of_squares, count):
    factor = jnp.minimum(1.0, 0.5 * lax.rsqrt(sum_of_squares / count + 1e-30))
    return [g * factor for g in gradients]


def solution(mesh):
    def step(x, dy, *arrays):
        weights, m, v = (arrays[i : i + 7] for i in (0, 7, 14))
        wq, wk, wv, wo, wg, wu, wd = weights
        cos, sin = tables(x.shape[1])
        layers = wq.shape[0]
        h, kept = x[0], []
        for n in range(layers):
            q, k, val = qkv(h, wq, wk, wv, cos, sin, n)
            o, lse, mid = attn(q, k, val, h, wo, n)
            kept.append((h, q, k, val, o, lse, mid))
            if n < layers - 1:
                h = mlp(mid, wg, wu, wd, n)
        by_h, mine = dy[0], [None] * layers
        for n in reversed(range(layers)):
            h, q, k, val, o, lse, mid = kept[n]
            dwg, dwu, dwd, dh = mlp_back(mid, by_h, wg, wu, wd, n)
            dwq, dwk, dwv, dwo, by_h = attn_back(h, dh, q, k, val, o, lse, wq, wk, wv, wo, cos, sin, n, n > 0)
            mine[n] = [lax.psum(g, "dp") for g in (dwq, dwk, dwv, dwo, dwg, dwu, dwd)]
        gradients = [jnp.stack([mine[n][i] for n in range(layers)]).astype(f32) for i in range(7)]
        gradients = clipped(gradients, sum(jnp.sum(g * g) for g in gradients), sum(g.size for g in gradients))
        new = [adamw(w.astype(f32), m, v, g) for w, m, v, g in zip(weights, m, v, gradients, strict=True)]
        return tuple(one[which] for which in range(3) for one in new)

    states, all_of = P(("rep", "dp"), None, None), P(None, None, None)
    return jax.shard_map(
        step, mesh=mesh, in_specs=(states, states) + (all_of,) * 21, out_specs=(P("rep", None, None),) * 21, check_vma=False,
    )
```

```python
import functools

import jax
import jax.numpy as jnp
from jax import lax
from jax.experimental import pallas as pl
from jax.experimental.pallas import tpu as pltpu
from jax.sharding import PartitionSpec as P


HEAD = 256
THETA = 10000
EPS = 1e-6
LOG2E = 1.4426950408889634
HIDDEN = -2e30
f32, bf16 = jnp.float32, jnp.bfloat16
VMEM = 67_043_328
ONE = pl.Buffered(1)
STAT = pl.BlockSpec((8, 128), lambda *_: (0, 0))


def dot(a, b, ca=1, cb=0):
    return lax.dot_general(a, b, (((ca,), (cb,)), ((), ())), preferred_element_type=f32)


def rows_of(i, n):
    return pl.ds(pl.multiple_of(i * n, n), n)


def inv_rms(h):
    return lax.rsqrt(jnp.mean(h * h, -1, keepdims=True) + EPS)


def norm_back(h, by_out):
    scale = inv_rms(h)
    return scale * (by_out - h * (scale * scale * jnp.mean(by_out * h, -1, keepdims=True)))


def cost(flops):
    return pl.CostEstimate(flops=flops, transcendentals=0, bytes_accessed=0)


def params(**more):
    return pltpu.CompilerParams(dimension_semantics=("arbitrary",), vmem_limit_bytes=VMEM, **more)


def _qkv(x_ref, wq_ref, wk_ref, wv_ref, cos_ref, sin_ref, q_ref, k_ref, v_ref):
    x = x_ref[...].astype(f32)
    a = (x * inv_rms(x)).astype(bf16)
    cos, sin = cos_ref[...], sin_ref[...]
    for w_ref, o_ref in ((wq_ref, q_ref), (wk_ref, k_ref)):
        t = dot(a, w_ref[...]).astype(bf16).astype(f32)
        half = HEAD // 2
        for h in range(t.shape[1] // HEAD):
            p, r = t[:, h * HEAD : h * HEAD + half], t[:, h * HEAD + half : (h + 1) * HEAD]
            o_ref[:, h * HEAD : h * HEAD + half] = (p * cos - r * sin).astype(bf16)
            o_ref[:, h * HEAD + half : (h + 1) * HEAD] = (r * cos + p * sin).astype(bf16)
    v_ref[...] = dot(a, wv_ref[...]).astype(bf16)


def qkv(x, wq, wk, wv, cos, sin, layer, tm=512):
    t, d = x.shape
    row = pl.BlockSpec((tm, d), lambda i: (i, 0))
    w = pl.BlockSpec((None, d, d), lambda i: (layer, 0, 0), pipeline_mode=ONE)
    tab = pl.BlockSpec((tm, HEAD // 2), lambda i: (i, 0))
    return pl.pallas_call(
        _qkv, grid=(t // tm,), in_specs=[row, w, w, w, tab, tab], out_specs=[row] * 3,
        out_shape=[jax.ShapeDtypeStruct((t, d), bf16)] * 3, compiler_params=params(), cost_estimate=cost(6 * t * d * d), name="qkv",
    )(x, wq, wk, wv, cos, sin)


def _attn(q_ref, k_ref, v_ref, x_ref, wo_ref, o_ref, lse_ref, h_ref, o_s, s_s, p_s, *, blk, scale):
    head = pl.program_id(0)
    t = q_ref.shape[0]
    e = scale * LOG2E
    vt = jnp.concatenate([v_ref[...].T, jnp.ones((16, t), bf16)], axis=0)
    for i in range(t // blk):
        here = pl.ds(i * blk, blk)
        q = q_ref[here, :]
        top = None
        for j in range(i + 1):
            s = dot(k_ref[j * blk : (j + 1) * blk, :], q, 1, 1)
            if i == j:
                gap = lax.broadcasted_iota(jnp.int32, (blk, blk), 1) - lax.broadcasted_iota(jnp.int32, (blk, blk), 0)
                s = jnp.where(gap >= 0, s, HIDDEN)
            s_s[j * blk : (j + 1) * blk, :] = s
            m = s.max(axis=0, keepdims=True)
            top = m if top is None else jnp.maximum(top, m)
        for j in range(i + 1):
            p_s[j * blk : (j + 1) * blk, :] = jnp.exp2((s_s[j * blk : (j + 1) * blk, :] - top) * e).astype(bf16)
        n = (i + 1) * blk
        mix = dot(vt[:, :n], p_s[:n, :])
        total = mix[HEAD : HEAD + 1, :]
        o = (mix[:HEAD, :] * (1 / total)).T.astype(bf16)
        o_ref[here, :] = o
        o_s[head, here, :] = o
        lse_ref[0, :, here] = top * scale + jnp.log(total)

    @pl.when(head == pl.num_programs(0) - 1)
    def _():
        def row(r, _):
            here = rows_of(r, 512)
            o = jnp.concatenate([o_s[n, here, :] for n in range(o_s.shape[0])], axis=1)
            h_ref[here, :] = (x_ref[here, :].astype(f32) + dot(o, wo_ref[...]).astype(bf16).astype(f32)).astype(bf16)
            return _

        lax.fori_loop(0, t // 512, row, None)


def attn(q, k, v, x, wo, layer, blk=512):
    t, d = x.shape
    heads = d // HEAD
    one = pl.BlockSpec((t, HEAD), lambda h: (0, h))
    full = pl.BlockSpec((t, d), lambda h: (0, 0), pipeline_mode=ONE)
    return pl.pallas_call(
        functools.partial(_attn, blk=blk, scale=HEAD**-0.5), grid=(heads,),
        in_specs=[one, one, one, full, pl.BlockSpec((None, d, d), lambda h: (layer, 0, 0), pipeline_mode=ONE)],
        out_specs=[one, pl.BlockSpec((1, 1, t), lambda h: (h, 0, 0)), full],
        out_shape=[jax.ShapeDtypeStruct((t, d), bf16), jax.ShapeDtypeStruct((heads, 1, t), f32), jax.ShapeDtypeStruct((t, d), bf16)],
        scratch_shapes=[pltpu.VMEM((heads, t, HEAD), bf16), pltpu.VMEM((t, blk), f32), pltpu.VMEM((t, blk), bf16)],
        compiler_params=params(), cost_estimate=cost(2 * t * d * d + 4 * t * t * d), name="attn",
    )(q, k, v, x, wo)


def _mlp(h_ref, wg_ref, wu_ref, wd_ref, y_ref, b_s, acc_s, *, tm):
    j = pl.program_id(0)
    t = h_ref.shape[0]

    @pl.when(j == 0)
    def _():
        def pre(r, _):
            here = rows_of(r, 256)
            h = h_ref[here, :].astype(f32)
            b_s[here, :] = (h * inv_rms(h)).astype(bf16)
            acc_s[here, :] = jnp.zeros((256, acc_s.shape[1]), f32)
            return _

        lax.fori_loop(0, t // 256, pre, None)

    def row(r, _):
        here = rows_of(r, tm)
        b = b_s[here, :]
        gate, up = dot(b, wg_ref[...]), dot(b, wu_ref[...])
        act = (gate * (1.0 / (1.0 + jnp.exp(-gate))) * up).astype(bf16)
        acc_s[here, :] += dot(act, wd_ref[...])
        return _

    lax.fori_loop(0, t // tm, row, None)

    @pl.when(j == pl.num_programs(0) - 1)
    def _():
        def post(r, _):
            here = rows_of(r, 256)
            y_ref[here, :] = (h_ref[here, :].astype(f32) + acc_s[here, :].astype(bf16).astype(f32)).astype(bf16)
            return _

        lax.fori_loop(0, t // 256, post, None)


def mlp(h, wg, wu, wd, layer, tf=512, tm=512):
    t, d = h.shape
    ff = wg.shape[2]
    full = pl.BlockSpec((t, d), lambda j: (0, 0), pipeline_mode=ONE)
    cols = pl.BlockSpec((None, d, tf), lambda j: (layer, 0, j))
    return pl.pallas_call(
        functools.partial(_mlp, tm=tm), grid=(ff // tf,),
        in_specs=[full, cols, cols, pl.BlockSpec((None, tf, d), lambda j: (layer, j, 0))], out_specs=full,
        out_shape=jax.ShapeDtypeStruct((t, d), bf16),
        scratch_shapes=[pltpu.VMEM((t, d), bf16), pltpu.VMEM((t, d), f32)],
        compiler_params=params(), cost_estimate=cost(6 * t * d * ff), name="mlp",
    )(h, wg, wu, wd)


MESH = pl.DeviceIdType.MESH


def place():
    i = lax.axis_index("dp")
    c, y, x = i % 2, i // 2 % 2, i // 4
    return (c, y, x), (i + 1 - 2 * c, i + 2 - 4 * y, i + 4 - 8 * x)


def meet():
    barrier = pltpu.get_barrier_semaphore()
    for other in place()[1]:
        pl.semaphore_signal(barrier, inc=1, device_id={"dp": other}, device_id_type=MESH)
    pl.semaphore_wait(barrier, 3)


def sending(src, dst, send, recv, to):
    return pltpu.make_async_remote_copy(src, dst, send, recv, device_id={"dp": to}, device_id_type=MESH)


class Scatter:
    def __init__(self, g, r0, p1, r1, p2, r2, s0, v0, s1, v1, s2, v2):
        self.g, self.r0, self.p1, self.r1, self.p2, self.r2 = g, r0, p1, r1, p2, r2
        self.s0, self.v0, self.s1, self.v1, self.s2, self.v2 = s0, v0, s1, v1, s2, v2
        self.rows, self.cols = g.shape[1:]
        self.at, self.to = place()

    @staticmethod
    def scratch(n, rows, cols, slots=1):
        half, eighth, last = rows // 2, rows // 8, rows // 16
        shapes = [(n, rows), (slots, n, half), (n, half), (n, 2, eighth), (n, 2, eighth), (n, 2, last)]
        one, two = pltpu.SemaphoreType.DMA((slots, n)), pltpu.SemaphoreType.DMA((n, 2))
        return [pltpu.VMEM((*shape, cols), bf16) for shape in shapes] + [one, one] + [two] * 4

    def _first(self, m, slot):
        rows = rows_of(1 - self.at[0], self.rows // 2)
        return sending(self.g.at[m, rows, :], self.r0.at[slot, m], self.s0.at[slot, m], self.v0.at[slot, m], self.to[0])

    def _second(self, m):
        n = self.rows // 8
        (_, y, x), (_, py, px) = self.at, self.to
        return [sending(self.p1.at[m, rows_of(2 * k + 1 - own, n), :], self.r1.at[m, k], self.s1.at[m, k], self.v1.at[m, k], to)
                for k, (own, to) in enumerate(((x, px), (y, py)))]

    def _third(self, m):
        n = self.rows // 16
        (_, y, x), (_, py, px) = self.at, self.to
        return [sending(self.p2.at[m, k, rows_of(1 - own, n), :], self.r2.at[m, k], self.s2.at[m, k], self.v2.at[m, k], to)
                for k, (own, to) in enumerate(((y, py), (x, px)))]

    def start(self, m, slot=0):
        self._first(m, slot).start()

    def cross_one(self, m, slot=0):
        half, step = self.rows // 2, 128
        self._first(m, slot).wait()

        def add(i, _):
            here = rows_of(i, step)
            own = self.g[m, rows_of(self.at[0] * (half // step) + i, step), :]
            self.p1[m, here, :] = (own.astype(f32) + self.r0[slot, m, here, :].astype(f32)).astype(bf16)
            return _

        lax.fori_loop(0, half // step, add, None)
        for copy in self._second(m):
            copy.start()

    def cross_two(self, m):
        _, y, x = self.at
        for copy in self._second(m):
            copy.wait()
        for k, own in enumerate((x, y)):
            term = self.p1[m, rows_of(2 * k + own, self.rows // 8), :]
            self.p2[m, k] = (term.astype(f32) + self.r1[m, k].astype(f32)).astype(bf16)
        for copy in self._third(m):
            copy.start()

    def finish(self, m, out, block, squares):
        _, y, x = self.at
        n = self.rows // 16
        for copy in self._third(m):
            copy.wait()
        for k, own in enumerate((y, x)):
            term = self.p2[m, k, rows_of(own, n), :]
            total = (term.astype(f32) + self.r2[m, k].astype(f32)).astype(bf16)
            out[block, m, k] = total
            wide = total.astype(f32)
            squares[...] += jnp.sum((wide * wide).reshape(n // 8, 8, self.cols // 128, 128), axis=(0, 2))


def sum_of_all(ref, got, send, recv):
    for k, other in enumerate(place()[1]):
        copy = sending(ref.at[k], got.at[k], send.at[k], recv.at[k], other)
        copy.start()
        copy.wait()
        ref[k + 1] = ref[k] + got[k]


def _mlp_back(h_ref, dy_ref, wg_ref, wu_ref, wd_ref, out_ref, sq_ref, dh_ref, b_s, bt_s, acc_s, at_s, dg_s, du_s, *comm, tm, dm):
    j, last = pl.program_id(0), pl.num_programs(0) - 1
    t, d = h_ref.shape
    tf = wg_ref.shape[1]
    sums = Scatter(*comm)

    @pl.when(j == 0)
    def _():
        meet()
        sq_ref[...] = jnp.zeros_like(sq_ref)

        def pre(r, _):
            here = rows_of(r, 256)
            h = h_ref[here, :].astype(f32)
            b = (h * inv_rms(h)).astype(bf16)
            b_s[here, :] = b
            bt_s[:, here] = b.T
            acc_s[here, :] = jnp.zeros((256, d), f32)
            return _

        lax.fori_loop(0, t // 256, pre, None)

    def row(r, _):
        here = rows_of(r, tm)
        b = b_s[here, :]
        gate, up = dot(b, wg_ref[...]), dot(b, wu_ref[...])
        da = dot(dy_ref[here, :], wd_ref[...], 1, 1).astype(bf16).astype(f32)
        s = 1.0 / (1.0 + jnp.exp(-gate))
        silu = gate * s
        at_s[:, here] = (silu * up).astype(bf16).T
        du_s[here, :] = (da * silu).astype(bf16)
        dg_s[here, :] = (da * up * (s * (1.0 + gate * (1.0 - s)))).astype(bf16)

        @pl.when((j > 0) & (r == 1))
        def _():
            sums.finish(0, out_ref, j - 1, sq_ref)
            sums.cross_two(2)

        @pl.when((j > 0) & (r == t // tm - 1))
        def _():
            sums.finish(1, out_ref, j - 1, sq_ref)
            sums.finish(2, out_ref, j - 1, sq_ref)

        return _

    lax.fori_loop(0, t // tm, row, None)
    for m, term in enumerate((dg_s, du_s)):

        def col(r, _):
            here = rows_of(r, dm)
            sums.g[m, here, :] = dot(bt_s[here, :], term[...]).astype(bf16)
            return _

        lax.fori_loop(0, d // dm, col, None)
        if m:
            sums.cross_one(m - 1)
        sums.start(m)
    for k in range(d // tf):
        sums.g[2, k * tf : (k + 1) * tf, :] = dot(at_s[...], dy_ref[:, k * tf : (k + 1) * tf]).astype(bf16)
    sums.cross_one(1)
    sums.start(2)

    def back(r, _):
        here = rows_of(r, tm)
        acc_s[here, :] += dot(dg_s[here, :], wg_ref[...], 1, 1) + dot(du_s[here, :], wu_ref[...], 1, 1)

        @pl.when(r == 1)
        def _():
            sums.cross_two(0)
            sums.cross_one(2)

        return _

    lax.fori_loop(0, t // tm, back, None)
    sums.cross_two(1)

    @pl.when(j == last)
    def _():
        def post(r, _):
            here = rows_of(r, 256)
            by_b = acc_s[here, :].astype(bf16).astype(f32)
            dh_ref[here, :] = (dy_ref[here, :].astype(f32) + norm_back(h_ref[here, :].astype(f32), by_b)).astype(bf16)
            return _

        lax.fori_loop(0, t // 256, post, None)
        sums.finish(0, out_ref, j, sq_ref)
        sums.cross_two(2)
        sums.finish(1, out_ref, j, sq_ref)
        sums.finish(2, out_ref, j, sq_ref)


def mlp_back(h, dy, wg, wu, wd, layer, tf=512, tm=512, dm=512):
    t, d = h.shape
    ff = wg.shape[2]
    full = pl.BlockSpec((t, d), lambda j: (0, 0), pipeline_mode=ONE)
    cols = pl.BlockSpec((None, d, tf), lambda j: (layer, 0, j))
    own = (ff // tf, 3, 2, d // 16, tf)
    return pl.pallas_call(
        functools.partial(_mlp_back, tm=tm, dm=dm), grid=(ff // tf,),
        in_specs=[full, full, cols, cols, pl.BlockSpec((None, tf, d), lambda j: (layer, j, 0))],
        out_specs=[pl.BlockSpec(own, lambda j: (0,) * 5, pipeline_mode=ONE), STAT, full],
        out_shape=[jax.ShapeDtypeStruct(own, bf16), jax.ShapeDtypeStruct((8, 128), f32), jax.ShapeDtypeStruct((t, d), bf16)],
        scratch_shapes=[pltpu.VMEM((t, d), bf16), pltpu.VMEM((d, t), bf16), pltpu.VMEM((t, d), f32), pltpu.VMEM((tf, t), bf16),
                        pltpu.VMEM((t, tf), bf16), pltpu.VMEM((t, tf), bf16)] + Scatter.scratch(3, d, tf),
        compiler_params=params(collective_id=layer, has_side_effects=True), cost_estimate=cost(16 * t * d * ff),
    )(h, dy, wg, wu, wd)


def _attn_back(x_ref, dh_ref, q_ref, k_ref, v_ref, o_ref, lse_ref, wq_ref, wk_ref, wv_ref, wo_ref, cos_ref, sin_ref, *refs, blk, scale, inner):
    if inner:
        out_ref, sq_ref, dx_ref, at_s, acc_s, do_s, delta_s, p_s, ds_s, dqt_s, dk_s, dv_s, g_s, *comm = refs
    else:
        one_ref, two_ref, three_ref, out_ref, all_ref, at_s, do_s, delta_s, p_s, ds_s, dqt_s, dk_s, dv_s, g_s, sq_ref, tot_s, got_s, *flags = refs
        flags, comm = flags[:2], flags[2:]
    head, last = pl.program_id(0), pl.num_programs(0) - 1
    t, d = x_ref.shape
    sums = Scatter(*comm)
    blocks, slot = range(4), head % 2
    n = t // blk
    e = scale * LOG2E

    @pl.when(head == 0)
    def _():
        meet()
        sq_ref[...] = jnp.zeros_like(sq_ref)

        def pre(r, _):
            here = rows_of(r, 256)
            h = x_ref[here, :].astype(f32)
            at_s[:, here] = (h * inv_rms(h)).astype(bf16).T
            if inner:
                acc_s[here, :] = jnp.zeros((256, d), f32)
            return _

        lax.fori_loop(0, t // 256, pre, None)

    for i in range(n):
        here = pl.ds(i * blk, blk)
        do = dot(dh_ref[here, :], wo_ref[...], 1, 1).astype(bf16)
        do_s[here, :] = do
        delta = jnp.sum(do.astype(f32) * o_ref[here, :].astype(f32), -1, keepdims=True)
        delta_s[:, here] = jnp.broadcast_to(delta, (blk, 128)).T[:8, :]

    @pl.when(head > 0)
    def _():
        for m in blocks:
            sums.cross_one(m, 1 - slot)

    dqt_s[...] = jnp.zeros_like(dqt_s)
    for j in range(n):
        kj, vj = k_ref[j * blk : (j + 1) * blk, :], v_ref[j * blk : (j + 1) * blk, :]
        for i in range(j, n):
            cols = pl.ds(i * blk, blk)
            s = dot(kj, q_ref[cols, :], 1, 1)
            dp = dot(vj, do_s[cols, :], 1, 1)
            p = jnp.exp2(s * e - lse_ref[0, :, cols] * LOG2E)
            if i == j:
                gap = lax.broadcasted_iota(jnp.int32, (blk, blk), 1) - lax.broadcasted_iota(jnp.int32, (blk, blk), 0)
                p = jnp.where(gap >= 0, p, 0.0)
            p_s[:, cols] = p.astype(bf16)
            ds_s[:, cols] = (p * (dp - delta_s[0:1, cols])).astype(bf16)
        seen = slice(j * blk, t)
        dv_s[j * blk : (j + 1) * blk, :] = dot(p_s[:, seen], do_s[seen, :]).astype(bf16)
        dk_s[j * blk : (j + 1) * blk, :] = dot(ds_s[:, seen], q_ref[seen, :])
        dqt_s[:, seen] += dot(kj.T, ds_s[:, seen])

    @pl.when(head > 0)
    def _():
        for m in blocks:
            sums.cross_two(m)

    half = HEAD // 2
    for i in range(n):
        here = pl.ds(i * blk, blk)
        cos, sin = cos_ref[here, :], sin_ref[here, :]
        for which, g in ((0, dqt_s[:, here].T), (1, dk_s[here, :])):
            g = (g * scale).astype(bf16).astype(f32)
            a, b = g[:, :half], g[:, half:]
            g_s[here, which * HEAD : which * HEAD + half] = (a * cos + b * sin).astype(bf16)
            g_s[here, which * HEAD + half : (which + 1) * HEAD] = (b * cos - a * sin).astype(bf16)

    ot = o_ref[...].T
    for k in range(d // HEAD):
        sums.g[3, k * HEAD : (k + 1) * HEAD, :] = dot(ot, dh_ref[:, k * HEAD : (k + 1) * HEAD]).astype(bf16)
    for m, term in enumerate((g_s[:, :HEAD], g_s[:, HEAD:], dv_s[...])):
        sums.g[m] = dot(at_s[...], term).astype(bf16)

    @pl.when(head > 0)
    def _():
        for m in blocks:
            sums.finish(m, out_ref, head - 1, sq_ref)

    for m in blocks:
        sums.start(m, slot)
    if inner:
        for i in range(n):
            here = pl.ds(i * blk, blk)
            acc_s[here, :] += (dot(g_s[here, :HEAD], wq_ref[...], 1, 1) + dot(g_s[here, HEAD:], wk_ref[...], 1, 1)
                               + dot(dv_s[here, :], wv_ref[...], 1, 1))

    @pl.when(head == last)
    def _():
        for m in blocks:
            sums.cross_one(m, slot)
        if inner:

            def post(r, _):
                here = rows_of(r, 256)
                by_a = acc_s[here, :].astype(bf16).astype(f32)
                dx_ref[here, :] = (dh_ref[here, :].astype(f32) + norm_back(x_ref[here, :].astype(f32), by_a)).astype(bf16)
                return _

            lax.fori_loop(0, t // 256, post, None)
        for m in blocks:
            sums.cross_two(m)
        for m in blocks:
            sums.finish(m, out_ref, head, sq_ref)
        if not inner:
            tot_s[0] = sq_ref[...] + one_ref[...] + two_ref[...] + three_ref[...]
            sum_of_all(tot_s, got_s, *flags)
            all_ref[...] = tot_s[tot_s.shape[0] - 1]


def attn_back(x, dh, q, k, v, o, lse, wq, wk, wv, wo, cos, sin, layer, squares, blk=512):
    t, d = x.shape
    heads = d // HEAD
    inner = squares is None
    full = pl.BlockSpec((t, d), lambda h: (0, 0), pipeline_mode=ONE)
    one = pl.BlockSpec((t, HEAD), lambda h: (0, h))
    cols = pl.BlockSpec((None, d, HEAD), lambda h: (layer, 0, h))
    tab = pl.BlockSpec((t, HEAD // 2), lambda h: (0, 0), pipeline_mode=ONE)
    own = (heads, 4, 2, d // 16, HEAD)
    stat = jax.ShapeDtypeStruct((8, 128), f32)
    flags = pltpu.SemaphoreType.DMA((3,))
    return pl.pallas_call(
        functools.partial(_attn_back, blk=blk, scale=HEAD**-0.5, inner=inner), grid=(heads,),
        in_specs=[full, full, one, one, one, one, pl.BlockSpec((1, 1, t), lambda h: (h, 0, 0)), cols, cols, cols,
                  pl.BlockSpec((None, HEAD, d), lambda h: (layer, h, 0)), tab, tab] + ([] if inner else [STAT] * 3),
        out_specs=[pl.BlockSpec(own, lambda h: (0,) * 5, pipeline_mode=ONE), STAT] + ([full] if inner else []),
        out_shape=[jax.ShapeDtypeStruct(own, bf16), stat] + ([jax.ShapeDtypeStruct((t, d), bf16)] if inner else []),
        scratch_shapes=[pltpu.VMEM((d, t), bf16)] + ([pltpu.VMEM((t, d), f32)] if inner else [])
        + [pltpu.VMEM((t, HEAD), bf16), pltpu.VMEM((8, t), f32), pltpu.VMEM((blk, t), bf16), pltpu.VMEM((blk, t), bf16),
           pltpu.VMEM((HEAD, t), f32), pltpu.VMEM((t, HEAD), f32), pltpu.VMEM((t, HEAD), bf16), pltpu.VMEM((t, 2 * HEAD), bf16)]
        + ([] if inner else [pltpu.VMEM((8, 128), f32), pltpu.VMEM((4, 8, 128), f32), pltpu.VMEM((3, 8, 128), f32), flags, flags])
        + Scatter.scratch(4, d, HEAD, 2),
        compiler_params=params(collective_id=2 + layer, has_side_effects=True), cost_estimate=cost(22 * t * d * d + 8 * t * t * d),
    )(x, dh, q, k, v, o, lse, wq, wk, wv, wo, cos, sin, *(squares or ()))


def tables(t):
    half, lane = HEAD // 2, 128
    by = THETA ** (-jnp.arange(half, dtype=f32) / half)
    high = (jnp.arange(t // lane, dtype=f32) * lane)[:, None, None] * by
    low = jnp.arange(lane, dtype=f32)[:, None] * by
    (ch, sh), (cl, sl) = lax.optimization_barrier(((jnp.cos(high), jnp.sin(high)), (jnp.cos(low), jnp.sin(low))))
    return (ch * cl - sh * sl).reshape(t, half), (sh * cl + ch * sl).reshape(t, half)


def owner(half, late, s):
    hi, lo = s // 2, s % 2
    x, y = hi + (lo - hi) * late, lo + (hi - lo) * late
    return x * 4 + y * 2 + half


def flat(g, which):
    _, blocks, _, _, n, cols = g.shape
    return pl.BlockSpec((1, blocks, 1, 1, n, cols), lambda r: (owner(r // 8, r // 4 % 2, r % 4), 0, which, r // 4 % 2, 0, 0))


def piece(g, index):
    def at(r):
        half, late, s, block, which = index(r)
        return owner(half, late, s), block, which, late, 0, 0

    return pl.BlockSpec((1, 1, 1, 1, *g.shape[4:]), at)


def update(refs, which, at, g, factor):
    n = len(refs) // 6
    w_ref, m_ref, v_ref, w_out, m_out, v_out = (refs[kind * n + which] for kind in range(6))
    g = g.astype(f32) * factor
    m = 0.9 * m_ref[at] + 0.1 * g
    v = 0.95 * v_ref[at] + 0.05 * g * g
    w = w_ref[at].astype(f32)
    w_out[at] = (w - 0.02 * (m * lax.rsqrt(v + 1e-8) + 0.1 * w)).astype(bf16)
    m_out[at] = m
    v_out[at] = v


def _adam(sq_ref, *refs, count, flats, pieces, arrays, cols):
    factor = jnp.minimum(1.0, 0.5 * lax.rsqrt(jnp.sum(sq_ref[...]) / count + 1e-30))
    n_flat, n_given = flats, flats + len(pieces)
    state = refs[n_given : n_given + arrays] + refs[len(refs) - arrays :]
    for which in range(n_flat):
        for k in range(refs[which].shape[1]):
            update(state, which, (slice(None), slice(k * cols, (k + 1) * cols)), refs[which][0, k, 0, 0], factor)
    for ref, (row, col) in zip(refs[n_flat:n_given], pieces):
        rows = ref.shape[4]
        at = slice(row * rows, (row + 1) * rows), slice(col * cols, (col + 1) * cols)
        update(state, n_flat, at, ref[0, 0, 0, 0], factor)


def adam(squares, g, arrays, layer, before, count):
    _, blocks, matrices, _, n, cols = g.shape
    d = arrays[0].shape[1]
    flats = matrices - 1
    tall = arrays[flats].shape[1] // (d // n)
    across = d // cols
    if tall == n:
        places = [(0, k) for k in range(across)]
        spec = [piece(g, lambda r, k=k: (k // 2, k % 2, r % 4, r // 4, flats)) for k in range(across)]
    else:
        places = [(s, k) for s in range(tall // n) for k in range(across)]
        spec = [piece(g, lambda r, s=s, k=k: (k, r % 2, s, r // 2, flats)) for s, k in places]
    kinds = [pl.BlockSpec((None, n, a.shape[2]), lambda r: (layer, r, 0)) for a in arrays[:flats]]
    kinds = (kinds + [pl.BlockSpec((None, tall, d), lambda r: (layer, r, 0))]) * 3
    given = [squares] + [g] * (flats + len(places)) + list(arrays)
    specs = [STAT] + [flat(g, which) for which in range(flats)] + spec + kinds
    aliases = {}
    if before is not None:
        aliases = {len(given) + i: i for i in range(len(arrays))}
        given += list(before)
        specs += [pl.BlockSpec(memory_space=pl.ANY)] * len(arrays)
    return pl.pallas_call(
        functools.partial(_adam, count=count, flats=flats, pieces=places, arrays=len(arrays), cols=cols), grid=(d // n,),
        in_specs=specs, out_specs=kinds, out_shape=[jax.ShapeDtypeStruct(a.shape, a.dtype) for a in arrays],
        input_output_aliases=aliases, compiler_params=params(), cost_estimate=cost(4000 * arrays[0].size), name="adam",
    )(*given)


def solution(mesh):
    def step(x, dy, *arrays):
        weights, m, v = (arrays[i : i + 7] for i in (0, 7, 14))
        wq, wk, wv, wo, wg, wu, wd = weights
        cos, sin = tables(x.shape[1])
        layers = wq.shape[0]
        h, kept = x[0], []
        for n in range(layers):
            q, k, val = qkv(h, wq, wk, wv, cos, sin, n)
            o, lse, mid = attn(q, k, val, h, wo, n)
            kept.append((h, q, k, val, o, lse, mid))
            if n < layers - 1:
                h = mlp(mid, wg, wu, wd, n)
        by_h, parts, squares = dy[0], [], []
        for n in reversed(range(layers)):
            h, q, k, val, o, lse, mid = kept[n]
            g_mlp, square, dh = mlp_back(mid, by_h, wg, wu, wd, n)
            squares.append(square)
            g_attn, square, *rest = attn_back(h, dh, q, k, val, o, lse, wq, wk, wv, wo, cos, sin, n, squares if n == 0 else None)
            squares.append(square)
            by_h = rest[0] if rest else None
            for a, b, own in ((4, 7, g_mlp), (0, 4, g_attn)):
                parts.append((n, a, b, lax.all_gather(own, "dp")))
        total, count = squares[-1], sum(w.size for w in weights)
        new = {0: None, 4: None}
        for n, a, b, g in parts:
            new[a] = adam(total, g, (*weights[a:b], *m[a:b], *v[a:b]), n, new[a], count)
        return tuple(one for i in range(3) for a, size in ((0, 4), (4, 3)) for one in new[a][size * i : size * (i + 1)])

    states, all_of = P(("rep", "dp"), None, None), P(None, None, None)
    return jax.shard_map(
        step, mesh=mesh, in_specs=(states, states) + (all_of,) * 21, out_specs=(P("rep", None, None),) * 21, check_vma=False,
    )
```

```python
import functools

import jax
import jax.numpy as jnp
from jax import lax
from jax.experimental import pallas as pl
from jax.experimental.pallas import tpu as pltpu
from jax.sharding import PartitionSpec as P


HEAD = 256
THETA = 10000
EPS = 1e-6
LOG2E = 1.4426950408889634
HIDDEN = -2e30
f32, bf16 = jnp.float32, jnp.bfloat16
VMEM = 67_043_328
ONE = pl.Buffered(1)
STAT = pl.BlockSpec((8, 128), lambda *_: (0, 0))


def dot(a, b, ca=1, cb=0):
    return lax.dot_general(a, b, (((ca,), (cb,)), ((), ())), preferred_element_type=f32)


def loop(n, body):
    lax.fori_loop(0, n, body, None)


def whole(*shape):
    return pl.BlockSpec(shape, lambda *_: (0,) * len(shape), pipeline_mode=ONE)


def rows_of(i, n):
    return pl.ds(pl.multiple_of(i * n, n), n)


def inv_rms(h):
    return lax.rsqrt(jnp.mean(h * h, -1, keepdims=True) + EPS)


def half_tanh(x):
    return 0.5 * jnp.tanh(0.5 * x)


def norm_back(h, by_out):
    scale = inv_rms(h)
    return scale * (by_out - h * (scale * scale * jnp.mean(by_out * h, -1, keepdims=True)))


def cost(flops):
    return pl.CostEstimate(flops=flops, transcendentals=0, bytes_accessed=0)


def params(**more):
    return pltpu.CompilerParams(dimension_semantics=("arbitrary",), vmem_limit_bytes=VMEM, **more)


def _qkv(x_ref, wq_ref, wk_ref, wv_ref, cos_ref, sin_ref, q_ref, k_ref, v_ref):
    x = x_ref[...].astype(f32)
    a = (x * inv_rms(x)).astype(bf16)
    cos, sin = cos_ref[...], sin_ref[...]
    for w_ref, o_ref in ((wq_ref, q_ref), (wk_ref, k_ref)):
        t = dot(a, w_ref[...]).astype(bf16).astype(f32)
        half = HEAD // 2
        for h in range(t.shape[1] // HEAD):
            p, r = t[:, h * HEAD : h * HEAD + half], t[:, h * HEAD + half : (h + 1) * HEAD]
            o_ref[:, h * HEAD : h * HEAD + half] = (p * cos - r * sin).astype(bf16)
            o_ref[:, h * HEAD + half : (h + 1) * HEAD] = (r * cos + p * sin).astype(bf16)
    v_ref[...] = dot(a, wv_ref[...]).astype(bf16)


def qkv(x, wq, wk, wv, cos, sin, layer, tm=512):
    t, d = x.shape
    row = pl.BlockSpec((tm, d), lambda i: (i, 0))
    w = pl.BlockSpec((None, d, d), lambda i: (layer, 0, 0), pipeline_mode=ONE)
    tab = pl.BlockSpec((tm, HEAD // 2), lambda i: (i, 0))
    return pl.pallas_call(
        _qkv, grid=(t // tm,), in_specs=[row, w, w, w, tab, tab], out_specs=[row] * 3,
        out_shape=[jax.ShapeDtypeStruct((t, d), bf16)] * 3, compiler_params=params(), cost_estimate=cost(6 * t * d * d), name="qkv",
    )(x, wq, wk, wv, cos, sin)


def _attn(q_ref, k_ref, v_ref, x_ref, wo_ref, o_ref, lse_ref, h_ref, o_s, s_s, p_s, *, blk, scale):
    head = pl.program_id(0)
    t = q_ref.shape[0]
    e = scale * LOG2E
    vt = jnp.concatenate([v_ref[...].T, jnp.ones((16, t), bf16)], axis=0)
    for i in range(t // blk):
        here = pl.ds(i * blk, blk)
        q = q_ref[here, :]
        top = None
        for j in range(i + 1):
            s = dot(k_ref[j * blk : (j + 1) * blk, :], q, 1, 1)
            if i == j:
                gap = lax.broadcasted_iota(jnp.int32, (blk, blk), 1) - lax.broadcasted_iota(jnp.int32, (blk, blk), 0)
                s = jnp.where(gap >= 0, s, HIDDEN)
            s_s[j * blk : (j + 1) * blk, :] = s
            m = s.max(axis=0, keepdims=True)
            top = m if top is None else jnp.maximum(top, m)
        for j in range(i + 1):
            p_s[j * blk : (j + 1) * blk, :] = jnp.exp2((s_s[j * blk : (j + 1) * blk, :] - top) * e).astype(bf16)
        n = (i + 1) * blk
        mix = dot(vt[:, :n], p_s[:n, :])
        total = mix[HEAD : HEAD + 1, :]
        o = (mix[:HEAD, :] * (1 / total)).T.astype(bf16)
        o_ref[here, :] = o
        o_s[head, here, :] = o
        lse_ref[0, :, here] = top * scale + jnp.log(total)

    @pl.when(head == pl.num_programs(0) - 1)
    def _():
        def row(r, _):
            here = rows_of(r, 512)
            o = jnp.concatenate([o_s[n, here, :] for n in range(o_s.shape[0])], axis=1)
            h_ref[here, :] = (x_ref[here, :].astype(f32) + dot(o, wo_ref[...]).astype(bf16).astype(f32)).astype(bf16)
            return _

        loop(t // 512, row)


def attn(q, k, v, x, wo, layer, blk=512):
    t, d = x.shape
    heads = d // HEAD
    one = pl.BlockSpec((t, HEAD), lambda h: (0, h))
    full = whole(t, d)
    return pl.pallas_call(
        functools.partial(_attn, blk=blk, scale=HEAD**-0.5), grid=(heads,),
        in_specs=[one, one, one, full, pl.BlockSpec((None, d, d), lambda h: (layer, 0, 0), pipeline_mode=ONE)],
        out_specs=[one, pl.BlockSpec((1, 1, t), lambda h: (h, 0, 0)), full],
        out_shape=[jax.ShapeDtypeStruct((t, d), bf16), jax.ShapeDtypeStruct((heads, 1, t), f32), jax.ShapeDtypeStruct((t, d), bf16)],
        scratch_shapes=[pltpu.VMEM((heads, t, HEAD), bf16), pltpu.VMEM((t, blk), f32), pltpu.VMEM((t, blk), bf16)],
        compiler_params=params(), cost_estimate=cost(2 * t * d * d + 4 * t * t * d), name="attn",
    )(q, k, v, x, wo)


def _mlp(h_ref, wg_ref, wu_ref, wd_ref, y_ref, gate_ref, up_ref, b_s, acc_s, *, tm):
    j = pl.program_id(0)
    t = h_ref.shape[0]

    @pl.when(j == 0)
    def _():
        def pre(r, _):
            here = rows_of(r, 256)
            h = h_ref[here, :].astype(f32)
            b_s[here, :] = (h * inv_rms(h)).astype(bf16)
            acc_s[here, :] = jnp.zeros((256, acc_s.shape[1]), f32)
            return _

        loop(t // 256, pre)

    def row(r, _):
        here = rows_of(r, tm)
        b = b_s[here, :]
        gate, up = dot(b, wg_ref[...]), dot(b, wu_ref[...])
        gate_ref[here, :], up_ref[here, :] = gate, up
        act = (gate * (half_tanh(gate) + 0.5) * up).astype(bf16)
        acc_s[here, :] += dot(act, wd_ref[...])
        return _

    loop(t // tm, row)

    @pl.when(j == pl.num_programs(0) - 1)
    def _():
        def post(r, _):
            here = rows_of(r, 256)
            y_ref[here, :] = (h_ref[here, :].astype(f32) + acc_s[here, :].astype(bf16).astype(f32)).astype(bf16)
            return _

        loop(t // 256, post)


def mlp(h, wg, wu, wd, layer, tf=512, tm=1024):
    t, d = h.shape
    ff = wg.shape[2]
    full = whole(t, d)
    cols = pl.BlockSpec((None, d, tf), lambda j: (layer, 0, j))
    return pl.pallas_call(
        functools.partial(_mlp, tm=tm), grid=(ff // tf,),
        in_specs=[full, cols, cols, pl.BlockSpec((None, tf, d), lambda j: (layer, j, 0))],
        out_specs=[full, pl.BlockSpec((None, t, tf), lambda j: (j, 0, 0)), pl.BlockSpec((None, t, tf), lambda j: (j, 0, 0))],
        out_shape=[jax.ShapeDtypeStruct((t, d), bf16)] + [jax.ShapeDtypeStruct((ff // tf, t, tf), f32)] * 2,
        scratch_shapes=[pltpu.VMEM((t, d), bf16), pltpu.VMEM((t, d), f32)],
        compiler_params=params(), cost_estimate=cost(6 * t * d * ff), name="mlp",
    )(h, wg, wu, wd)


MESH = pl.DeviceIdType.MESH


def place():
    i = lax.axis_index("dp")
    c, y, x = i % 2, i // 2 % 2, i // 4
    return (c, y, x), (i + 1 - 2 * c, i + 2 - 4 * y, i + 4 - 8 * x)


def meet():
    barrier = pltpu.get_barrier_semaphore()
    for other in place()[1]:
        pl.semaphore_signal(barrier, inc=1, device_id={"dp": other}, device_id_type=MESH)
    pl.semaphore_wait(barrier, 3)


def sending(src, dst, send, recv, to):
    return pltpu.make_async_remote_copy(src, dst, send, recv, device_id={"dp": to}, device_id_type=MESH)


class Scatter:
    def __init__(self, g, r0, p1, r1, p2, r2, s0, v0, s1, v1, s2, v2, more=()):
        self.terms = [g.at[m] for m in range(g.shape[0])] + list(more)
        self.g, self.r0, self.p1, self.r1, self.p2, self.r2 = g, r0, p1, r1, p2, r2
        self.s0, self.v0, self.s1, self.v1, self.s2, self.v2 = s0, v0, s1, v1, s2, v2
        self.rows, self.cols = g.shape[1:]
        self.at, self.to = place()

    @staticmethod
    def scratch(n, rows, cols, slots=1, more=0):
        mine, n = n, n + more
        half, eighth, last = rows // 2, rows // 8, rows // 16
        shapes = [(mine, rows), (slots, n, half), (n, half), (n, 2, eighth), (n, 2, eighth), (n, 2, last)]
        one, two = pltpu.SemaphoreType.DMA((slots, n)), pltpu.SemaphoreType.DMA((n, 2))
        return [pltpu.VMEM((*shape, cols), bf16) for shape in shapes] + [one, one] + [two] * 4

    def _first(self, m, slot):
        rows = rows_of(1 - self.at[0], self.rows // 2)
        return sending(self.terms[m].at[rows, :], self.r0.at[slot, m], self.s0.at[slot, m], self.v0.at[slot, m], self.to[0])

    def _second(self, m):
        n = self.rows // 8
        (_, y, x), (_, py, px) = self.at, self.to
        return [sending(self.p1.at[m, rows_of(2 * k + 1 - own, n), :], self.r1.at[m, k], self.s1.at[m, k], self.v1.at[m, k], to)
                for k, (own, to) in enumerate(((x, px), (y, py)))]

    def _third(self, m):
        n = self.rows // 16
        (_, y, x), (_, py, px) = self.at, self.to
        return [sending(self.p2.at[m, k, rows_of(1 - own, n), :], self.r2.at[m, k], self.s2.at[m, k], self.v2.at[m, k], to)
                for k, (own, to) in enumerate(((y, py), (x, px)))]

    def start(self, m, slot=0):
        self._first(m, slot).start()

    def cross_one(self, m, slot=0):
        half, step = self.rows // 2, 128
        self._first(m, slot).wait()

        def add(i, _):
            here = rows_of(i, step)
            own = self.terms[m][rows_of(self.at[0] * (half // step) + i, step), :]
            self.p1[m, here, :] = (own.astype(f32) + self.r0[slot, m, here, :].astype(f32)).astype(bf16)
            return _

        loop(half // step, add)
        for copy in self._second(m):
            copy.start()

    def cross_two(self, m):
        _, y, x = self.at
        for copy in self._second(m):
            copy.wait()
        for k, own in enumerate((x, y)):
            term = self.p1[m, rows_of(2 * k + own, self.rows // 8), :]
            self.p2[m, k] = (term.astype(f32) + self.r1[m, k].astype(f32)).astype(bf16)
        for copy in self._third(m):
            copy.start()

    def finish(self, m, out, squares):
        _, y, x = self.at
        n = self.rows // 16
        for copy in self._third(m):
            copy.wait()
        for k, own in enumerate((y, x)):
            term = self.p2[m, k, rows_of(own, n), :]
            total = (term.astype(f32) + self.r2[m, k].astype(f32)).astype(bf16)
            out[k] = total
            wide = total.astype(f32)
            squares[...] += jnp.sum((wide * wide).reshape(n // 8, 8, self.cols // 128, 128), axis=(0, 2))


def sum_of_all(ref, got, send, recv):
    for k, other in enumerate(place()[1]):
        copy = sending(ref.at[k], got.at[k], send.at[k], recv.at[k], other)
        copy.start()
        copy.wait()
        ref[k + 1] = ref[k] + got[k]


def _mlp_back(h_ref, dy_ref, wg_ref, wu_ref, wd_ref, *refs, tm, saved):
    if saved:
        gate_ref, up_ref, more_ref, out_ref, own_ref, sq_ref, dh_ref, gu_s, gu_sem, acc_s, bt_s, at_s, dg_s, du_s, *comm = refs
    else:
        out_ref, sq_ref, dh_ref, b_s, acc_s, bt_s, at_s, dg_s, du_s, *comm = refs
    j, last = pl.program_id(0), pl.num_programs(0) - 1
    t, d = h_ref.shape
    tf = wg_ref.shape[1]
    steps = t // tm
    sums = Scatter(*comm, [more_ref.at[0]] if saved else [])
    done = lambda m, tile: sums.finish(m, out_ref.at[tile, m], sq_ref)

    def fetch(tile, r):
        return [pltpu.make_async_copy(ref.at[tile, rows_of(r, tm), :], gu_s.at[r % 2, i], gu_sem.at[r % 2, i])
                for i, ref in enumerate((gate_ref, up_ref))]

    @pl.when(j == 0)
    def _():
        if saved:
            for copy in fetch(0, 0):
                copy.start()
        meet()
        sq_ref[...] = jnp.zeros_like(sq_ref)

        def pre(r, _):
            here = rows_of(r, 256)
            h = h_ref[here, :].astype(f32)
            b = (h * inv_rms(h)).astype(bf16)
            if not saved:
                b_s[here, :] = b
            bt_s[:, here] = b.T
            acc_s[here, :] = jnp.zeros((256, d), f32)
            return _

        loop(t // 256, pre)

    if saved:
        sums.start(3)

    def row(r, _):
        here = rows_of(r, tm)
        if saved:
            tile, following = j + (r + 1) // steps, (r + 1) % steps

            @pl.when(tile <= last)
            def _():
                for copy in fetch(tile, following):
                    copy.start()

            for copy in fetch(j, r):
                copy.wait()
            gate, up = gu_s[r % 2, 0], gu_s[r % 2, 1]
        else:
            b = b_s[here, :]
            gate, up = dot(b, wg_ref[...]), dot(b, wu_ref[...])
        da = dot(dy_ref[here, :], wd_ref[...], 1, 1).astype(bf16).astype(f32)
        at = half_tanh(gate)
        s = at + 0.5
        silu = gate * s
        at_s[:, here] = (silu * up).astype(bf16).T
        du = (da * silu).astype(bf16)
        dg = (da * up * (s + silu * (0.5 - at))).astype(bf16)
        du_s[here, :] = du
        dg_s[here, :] = dg
        acc_s[here, :] += dot(dg, wg_ref[...], 1, 1) + dot(du, wu_ref[...], 1, 1)

        @pl.when((j > 0) & (r == 0))
        def _():
            sums.cross_one(2)
            sums.cross_two(0)

        if saved:

            @pl.when(r == 1)
            def _():
                sums.cross_one(3)

        @pl.when((j > 0) & (r == 2))
        def _():
            sums.cross_two(1)

        return _

    loop(steps, row)

    @pl.when(j > 0)
    def _():
        sums.cross_two(2)
        done(0, j - 1)

    if saved:
        sums.cross_two(3)
    for m, term in enumerate((dg_s, du_s)):
        sums.g[m] = dot(bt_s[...], term[...]).astype(bf16)
        if m:
            sums.cross_one(0)
        sums.start(m)

        @pl.when(j > 0)
        def _():
            done(m + 1, j - 1)

    if saved:
        sums.finish(3, own_ref.at[j], sq_ref)

    for k in range(d // tf):
        sums.g[2, k * tf : (k + 1) * tf, :] = dot(at_s[...], dy_ref[:, k * tf : (k + 1) * tf]).astype(bf16)
    sums.cross_one(1)
    sums.start(2)

    @pl.when(j == last)
    def _():
        def post(r, _):
            here = rows_of(r, 256)
            by_b = acc_s[here, :].astype(bf16).astype(f32)
            dh_ref[here, :] = (dy_ref[here, :].astype(f32) + norm_back(h_ref[here, :].astype(f32), by_b)).astype(bf16)
            return _

        loop(t // 256, post)
        sums.cross_one(2)
        sums.cross_two(0)
        sums.cross_two(1)
        done(0, j)
        sums.cross_two(2)
        done(1, j)
        done(2, j)


def mlp_back(h, dy, wg, wu, wd, layer, saved=(), tf=512, tm=512):
    t, d = h.shape
    ff = wg.shape[2]
    tiles = ff // tf
    full = whole(t, d)
    cols = pl.BlockSpec((None, d, tf), lambda j: (layer, 0, j))
    own, more = (tiles, 3, 2, d // 16, tf), (tiles, 2, d // 16, tf)
    results = [own, more] if saved else [own]
    given = [pl.BlockSpec(memory_space=pl.ANY)] * 2 + [pl.BlockSpec((1, d, tf), lambda j: (j, 0, 0))] if saved else []
    first = [pltpu.VMEM((2, 2, tm, tf), f32), pltpu.SemaphoreType.DMA((2, 2))] if saved else [pltpu.VMEM((t, d), bf16)]
    return pl.pallas_call(
        functools.partial(_mlp_back, tm=tm, saved=bool(saved)), grid=(tiles,),
        in_specs=[full, full, cols, cols, pl.BlockSpec((None, tf, d), lambda j: (layer, j, 0))] + given,
        out_specs=[whole(*shape) for shape in results] + [STAT, full],
        out_shape=[jax.ShapeDtypeStruct(shape, bf16) for shape in results] + [jax.ShapeDtypeStruct((8, 128), f32), jax.ShapeDtypeStruct((t, d), bf16)],
        scratch_shapes=first + [pltpu.VMEM((t, d), f32)] + [pltpu.VMEM(shape, bf16) for shape in ((d, t), (tf, t), (t, tf), (t, tf))] + Scatter.scratch(3, d, tf, more=int(bool(saved))),
        compiler_params=params(collective_id=layer, has_side_effects=True), cost_estimate=cost(16 * t * d * ff),
    )(h, dy, wg, wu, wd, *saved)


def _attn_back(x_ref, dh_ref, q_ref, k_ref, v_ref, o_ref, lse_ref, wq_ref, wk_ref, wv_ref, wo_ref, cos_ref, sin_ref, *refs, blk, scale, inner):
    if inner:
        grad_ref, dx_ref, at_s, acc_s, do_s, delta_s, p_s, ds_s, dqt_s, dk_s, dv_s, g_s = refs
    else:
        one_ref, two_ref, out_ref, all_ref, at_s, do_s, delta_s, p_s, ds_s, dqt_s, dk_s, dv_s, g_s, sq_ref, tot_s, got_s, *flags = refs
        sums = Scatter(*flags[2:])
        grad_ref = sums.g
    head, last = pl.program_id(0), pl.num_programs(0) - 1
    t, d = x_ref.shape
    blocks, slot = range(2), head % 2
    n = t // blk
    e = scale * LOG2E

    @pl.when(head == 0)
    def _():
        if not inner:
            meet()
            sq_ref[...] = jnp.zeros_like(sq_ref)

        def pre(r, _):
            here = rows_of(r, 256)
            h = x_ref[here, :].astype(f32)
            at_s[:, here] = (h * inv_rms(h)).astype(bf16).T
            if inner:
                acc_s[here, :] = jnp.zeros((256, d), f32)
            return _

        loop(t // 256, pre)

    for i in range(n):
        here = pl.ds(i * blk, blk)
        do = dot(dh_ref[here, :], wo_ref[...], 1, 1).astype(bf16)
        do_s[here, :] = do
        delta = jnp.sum(do.astype(f32) * o_ref[here, :].astype(f32), -1, keepdims=True)
        delta_s[:, here] = jnp.broadcast_to(delta, (blk, 128)).T[:8, :]

    if not inner:

        @pl.when(head > 0)
        def _():
            for m in blocks:
                sums.cross_one(m, 1 - slot)

    dqt_s[...] = jnp.zeros_like(dqt_s)
    for j in range(n):
        kj, vj = k_ref[j * blk : (j + 1) * blk, :], v_ref[j * blk : (j + 1) * blk, :]
        for i in range(j, n):
            cols = pl.ds(i * blk, blk)
            s = dot(kj, q_ref[cols, :], 1, 1)
            dp = dot(vj, do_s[cols, :], 1, 1)
            p = jnp.exp2(s * e - lse_ref[0, :, cols] * LOG2E)
            if i == j:
                gap = lax.broadcasted_iota(jnp.int32, (blk, blk), 1) - lax.broadcasted_iota(jnp.int32, (blk, blk), 0)
                p = jnp.where(gap >= 0, p, 0.0)
            p_s[:, cols] = p.astype(bf16)
            ds_s[:, cols] = (p * (dp - delta_s[0:1, cols])).astype(bf16)
        seen = slice(j * blk, t)
        dv_s[j * blk : (j + 1) * blk, :] = dot(p_s[:, seen], do_s[seen, :]).astype(bf16)
        dk_s[j * blk : (j + 1) * blk, :] = dot(ds_s[:, seen], q_ref[seen, :])
        dqt_s[:, seen] += dot(kj.T, ds_s[:, seen])

    if not inner:

        @pl.when(head > 0)
        def _():
            for m in blocks:
                sums.cross_two(m)

    half = HEAD // 2
    for i in range(n):
        here = pl.ds(i * blk, blk)
        cos, sin = cos_ref[here, :], sin_ref[here, :]
        for which, g in ((0, dqt_s[:, here].T), (1, dk_s[here, :])):
            g = (g * scale).astype(bf16).astype(f32)
            a, b = g[:, :half], g[:, half:]
            g_s[here, which * HEAD : which * HEAD + half] = (a * cos + b * sin).astype(bf16)
            g_s[here, which * HEAD + half : (which + 1) * HEAD] = (b * cos - a * sin).astype(bf16)

    ot = o_ref[...].T
    for k in range(d // HEAD):
        grad_ref[1, k * HEAD : (k + 1) * HEAD, HEAD:] = dot(ot, dh_ref[:, k * HEAD : (k + 1) * HEAD]).astype(bf16)
    grad_ref[0] = dot(at_s[...], g_s[...]).astype(bf16)
    grad_ref[1, :, :HEAD] = dot(at_s[...], dv_s[...]).astype(bf16)
    if inner:
        for i in range(n):
            here = pl.ds(i * blk, blk)
            acc_s[here, :] += (dot(g_s[here, :HEAD], wq_ref[...], 1, 1) + dot(g_s[here, HEAD:], wk_ref[...], 1, 1)
                               + dot(dv_s[here, :], wv_ref[...], 1, 1))

        @pl.when(head == last)
        def _():
            def post(r, _):
                here = rows_of(r, 256)
                by_a = acc_s[here, :].astype(bf16).astype(f32)
                dx_ref[here, :] = (dh_ref[here, :].astype(f32) + norm_back(x_ref[here, :].astype(f32), by_a)).astype(bf16)
                return _

            loop(t // 256, post)

        return

    @pl.when(head > 0)
    def _():
        for m in blocks:
            sums.finish(m, out_ref.at[head - 1, m], sq_ref)

    for m in blocks:
        sums.start(m, slot)

    @pl.when(head == last)
    def _():
        for m in blocks:
            sums.cross_one(m, slot)
        for m in blocks:
            sums.cross_two(m)
        for m in blocks:
            sums.finish(m, out_ref.at[head, m], sq_ref)
        tot_s[0] = sq_ref[...] + one_ref[...] + two_ref[...]
        sum_of_all(tot_s, got_s, *flags[:2])
        all_ref[...] = tot_s[tot_s.shape[0] - 1]


def attn_back(x, dh, q, k, v, o, lse, wq, wk, wv, wo, cos, sin, layer, squares, blk=512):
    t, d = x.shape
    heads = d // HEAD
    inner = squares is None
    full = whole(t, d)
    one = pl.BlockSpec((t, HEAD), lambda h: (0, h))
    cols = pl.BlockSpec((None, d, HEAD), lambda h: (layer, 0, h))
    tab = whole(t, HEAD // 2)
    own, stat = (heads, 2, 2, d // 16, 2 * HEAD), (8, 128)
    flags = pltpu.SemaphoreType.DMA((3,))
    heads_first = [pltpu.VMEM((t, HEAD), bf16), pltpu.VMEM((8, t), f32), pltpu.VMEM((blk, t), bf16), pltpu.VMEM((blk, t), bf16),
                   pltpu.VMEM((HEAD, t), f32), pltpu.VMEM((t, HEAD), f32), pltpu.VMEM((t, HEAD), bf16), pltpu.VMEM((t, 2 * HEAD), bf16)]
    if inner:
        more = []
        outs = [pl.BlockSpec((2, d, 2 * HEAD), lambda h: (h, 0, 0)), full]
        shapes = [jax.ShapeDtypeStruct((2 * heads, d, 2 * HEAD), bf16), jax.ShapeDtypeStruct((t, d), bf16)]
        scratch = [pltpu.VMEM((d, t), bf16), pltpu.VMEM((t, d), f32)] + heads_first
        comm = {}
    else:
        more = [STAT] * len(squares)
        outs = [whole(*own), STAT]
        shapes = [jax.ShapeDtypeStruct(own, bf16), jax.ShapeDtypeStruct(stat, f32)]
        scratch = [pltpu.VMEM((d, t), bf16)] + heads_first + [pltpu.VMEM(stat, f32), pltpu.VMEM((4, *stat), f32), pltpu.VMEM((3, *stat), f32)]
        scratch += [flags, flags] + Scatter.scratch(2, d, 2 * HEAD, 2)
        comm = {"collective_id": 2, "has_side_effects": True}
    return pl.pallas_call(
        functools.partial(_attn_back, blk=blk, scale=HEAD**-0.5, inner=inner), grid=(heads,),
        in_specs=[full, full, one, one, one, one, pl.BlockSpec((1, 1, t), lambda h: (h, 0, 0)), cols, cols, cols,
                  pl.BlockSpec((None, HEAD, d), lambda h: (layer, h, 0)), tab, tab] + more,
        out_specs=outs, out_shape=shapes, scratch_shapes=scratch,
        compiler_params=params(**comm), cost_estimate=cost(22 * t * d * d + 8 * t * t * d),
    )(x, dh, q, k, v, o, lse, wq, wk, wv, wo, cos, sin, *(squares or ()))


def tables(t):
    half, lane = HEAD // 2, 128
    by = THETA ** (-jnp.arange(half, dtype=f32) / half)
    high = (jnp.arange(t // lane, dtype=f32) * lane)[:, None, None] * by
    low = jnp.arange(lane, dtype=f32)[:, None] * by
    (ch, sh), (cl, sl) = lax.optimization_barrier(((jnp.cos(high), jnp.sin(high)), (jnp.cos(low), jnp.sin(low))))
    return (ch * cl - sh * sl).reshape(t, half), (sh * cl + ch * sl).reshape(t, half)


def owner(half, late, s):
    hi, lo = s // 2, s % 2
    x, y = hi + (lo - hi) * late, lo + (hi - lo) * late
    return x * 4 + y * 2 + half


def flat(g, which, cols):
    _, blocks, _, _, n, wide = g.shape
    each = wide // cols
    return pl.BlockSpec((1, blocks, 1, 1, n, cols),
                        lambda r: (owner(r // 8, r // 4 % 2, r % 4), 0, which // each, r // 4 % 2, 0, which % each))


def piece(g, which, cols, index):
    each = g.shape[5] // cols

    def at(r):
        half, late, s, block = index(r)
        return owner(half, late, s), block, which // each, late, 0, which % each

    return pl.BlockSpec((1, 1, 1, 1, g.shape[4], cols), at)


def update(refs, which, at, g, factor):
    n = len(refs) // 6
    w_ref, m_ref, v_ref, w_out, m_out, v_out = (refs[kind * n + which] for kind in range(6))
    g = g.astype(f32) * factor
    m = 0.9 * m_ref[at] + 0.1 * g
    v = 0.95 * v_ref[at] + 0.05 * g * g
    w = w_ref[at].astype(f32)
    w_out[at] = (w - 0.02 * (m * lax.rsqrt(v + 1e-8) + 0.1 * w)).astype(bf16)
    m_out[at] = m
    v_out[at] = v


def _adam(sq_ref, *refs, count, flats, pieces, arrays, cols):
    factor = jnp.minimum(1.0, 0.5 * lax.rsqrt(jnp.sum(sq_ref[...]) / count + 1e-30))
    n_flat, n_given = flats, flats + len(pieces)
    state = refs[n_given : n_given + arrays] + refs[len(refs) - arrays :]
    for which in range(n_flat):
        for k in range(refs[which].shape[1]):
            update(state, which, (slice(None), slice(k * cols, (k + 1) * cols)), refs[which][0, k, 0, 0], factor)
    for ref, (row, col) in zip(refs[n_flat:n_given], pieces):
        rows = ref.shape[4]
        at = slice(row * rows, (row + 1) * rows), slice(col * cols, (col + 1) * cols)
        update(state, n_flat, at, ref[0, 0, 0, 0], factor)


def adam(squares, g, arrays, layer, before, count):
    n = g.shape[4]
    d = arrays[0].shape[1]
    flats = len(arrays) // 3 - 1
    cols = g.shape[2] * g.shape[5] // (flats + 1)
    tall = arrays[flats].shape[1] // (d // n)
    across = d // cols
    if tall == n:
        places = [(0, k) for k in range(across)]
        spec = [piece(g, flats, cols, lambda r, k=k: (k // 2, k % 2, r % 4, r // 4)) for k in range(across)]
    else:
        places = [(s, k) for s in range(tall // n) for k in range(across)]
        spec = [piece(g, flats, cols, lambda r, s=s, k=k: (k, r % 2, s, r // 2)) for s, k in places]
    kinds = [pl.BlockSpec((None, n, a.shape[2]), lambda r: (layer, r, 0)) for a in arrays[:flats]]
    kinds = (kinds + [pl.BlockSpec((None, tall, d), lambda r: (layer, r, 0))]) * 3
    given = [squares] + [g] * (flats + len(places)) + list(arrays)
    specs = [STAT] + [flat(g, which, cols) for which in range(flats)] + spec + kinds
    aliases = {}
    if before is not None:
        aliases = {len(given) + i: i for i in range(len(arrays))}
        given += list(before)
        specs += [pl.BlockSpec(memory_space=pl.ANY)] * len(arrays)
    return pl.pallas_call(
        functools.partial(_adam, count=count, flats=flats, pieces=places, arrays=len(arrays), cols=cols), grid=(d // n,),
        in_specs=specs, out_specs=kinds, out_shape=[jax.ShapeDtypeStruct(a.shape, a.dtype) for a in arrays],
        input_output_aliases=aliases, compiler_params=params(), cost_estimate=cost(4000 * arrays[0].size), name="adam",
    )(*given)


def solution(mesh):
    def step(x, dy, *arrays):
        weights, m, v = (arrays[i : i + 7] for i in (0, 7, 14))
        wq, wk, wv, wo, wg, wu, wd = weights
        cos, sin = tables(x.shape[1])
        layers = wq.shape[0]
        h, kept = x[0], []
        for n in range(layers):
            q, k, val = qkv(h, wq, wk, wv, cos, sin, n)
            o, lse, mid = attn(q, k, val, h, wo, n)
            kept.append((h, q, k, val, o, lse, mid))
            if n < layers - 1:
                h, *saved = mlp(mid, wg, wu, wd, n)
        parts = []

        def gather(n, a, b, own):
            parts.append((n, a, b, lax.all_gather(own, "dp")))

        h, q, k, val, o, lse, mid = kept[1]
        own, square_1, dh = mlp_back(mid, dy[0], wg, wu, wd, 1)
        gather(1, 4, 7, own)
        terms, by_h = attn_back(h, dh, q, k, val, o, lse, wq, wk, wv, wo, cos, sin, 1, None)
        h, q, k, val, o, lse, mid = kept[0]
        own, more, square_0, dh = mlp_back(mid, by_h, wg, wu, wd, 0, (*saved, terms))
        gather(1, 0, 4, more.reshape(-1, 2, *more.shape[1:]))
        gather(0, 4, 7, own)
        own, total = attn_back(h, dh, q, k, val, o, lse, wq, wk, wv, wo, cos, sin, 0, (square_1, square_0))
        gather(0, 0, 4, own)
        count = sum(w.size for w in weights)
        new = {0: None, 4: None}
        for n, a, b, g in parts:
            new[a] = adam(total, g, (*weights[a:b], *m[a:b], *v[a:b]), n, new[a], count)
        return tuple(one for i in range(3) for a, size in ((0, 4), (4, 3)) for one in new[a][size * i : size * (i + 1)])

    states, all_of = P(("rep", "dp"), None, None), P(None, None, None)
    return jax.shard_map(
        step, mesh=mesh, in_specs=(states, states) + (all_of,) * 21, out_specs=(P("rep", None, None),) * 21, check_vma=False,
    )
```

```python
import functools

import jax
import jax.numpy as jnp
from jax import lax
from jax.experimental import pallas as pl
from jax.experimental.pallas import tpu as pltpu
from jax.sharding import PartitionSpec as P


HEAD = 256
STRIP = 256
THETA = 10000
EPS = 1e-6
LOG2E = 1.4426950408889634
HIDDEN = -2e30
SCALE = HEAD**-0.5
f32, bf16 = jnp.float32, jnp.bfloat16
VMEM = 67_043_328
ONE = pl.Buffered(1)
STAT = pl.BlockSpec((8, 128), lambda *_: (0, 0))


def dot(a, b, ca=1, cb=0):
    return lax.dot_general(a, b, (((ca,), (cb,)), ((), ())), preferred_element_type=f32)


def loop(n, body):
    lax.fori_loop(0, n, body, None)


def whole(*shape):
    return pl.BlockSpec(shape, lambda *_: (0,) * len(shape), pipeline_mode=ONE)


def rows_of(i, n):
    return pl.ds(pl.multiple_of(i * n, n), n)


def inv_rms(h):
    return lax.rsqrt(jnp.mean(h * h, -1, keepdims=True) + EPS)


def half_tanh(x):
    return 0.5 * jnp.tanh(0.5 * x)


def norm_back(h, by_out):
    scale = inv_rms(h)
    return scale * (by_out - h * (scale * scale * jnp.mean(by_out * h, -1, keepdims=True)))


def cost(flops):
    return pl.CostEstimate(flops=flops, transcendentals=0, bytes_accessed=0)


def params(**more):
    return pltpu.CompilerParams(dimension_semantics=("arbitrary",), vmem_limit_bytes=VMEM, **more)


def _heads(x_ref, wq_ref, wk_ref, wv_ref, wo_ref, cos_ref, sin_ref, q_ref, k_ref, v_ref, o_ref, lse_ref, h_ref, a_s, t_s, o_s, s_s, p_s, *, blk, scale):
    step, last = pl.program_id(0), pl.num_programs(0) - 1
    t = x_ref.shape[0]
    n, half, e = t // blk, HEAD // 2, scale * LOG2E
    rows = [slice(i * blk, (i + 1) * blk) for i in range(n)]

    def project(slot, i):
        a, cos, sin = a_s[rows[i], :], cos_ref[rows[i], :], sin_ref[rows[i], :]
        for which, (w_ref, out_ref) in enumerate(((wq_ref, q_ref), (wk_ref, k_ref), (wv_ref, v_ref))):
            r = dot(a, w_ref[...]).astype(bf16)
            if which < 2:
                p, m = r[:, :half].astype(f32), r[:, half:].astype(f32)
                r = jnp.concatenate([p * cos - m * sin, m * cos + p * sin], axis=1).astype(bf16)
            out_ref[rows[i], :] = r
            t_s[slot, which, rows[i], :] = r

    def score(slot, i):
        q, top = t_s[slot, 0, rows[i], :], None
        for j in range(i + 1):
            s = dot(t_s[slot, 1, rows[j], :], q, 1, 1)
            if i == j:
                gap = lax.broadcasted_iota(jnp.int32, (blk, blk), 1) - lax.broadcasted_iota(jnp.int32, (blk, blk), 0)
                s = jnp.where(gap >= 0, s, HIDDEN)
            s_s[i % 2, rows[j], :] = s
            m = s.max(axis=0, keepdims=True)
            top = m if top is None else jnp.maximum(top, m)
        return top

    def weigh(i, vt, top):
        for j in range(i + 1):
            p_s[rows[j], :] = jnp.exp2((s_s[i % 2, rows[j], :] - top) * e).astype(bf16)
        seen = (i + 1) * blk
        mix = dot(vt[:, :seen], p_s[:seen, :])
        total = mix[HEAD : HEAD + 1, :]
        o = (mix[:HEAD, :] * (1 / total)).T.astype(bf16)
        o_ref[rows[i], :] = o
        o_s[step - 1, rows[i], :] = o
        lse_ref[0, :, rows[i]] = top * scale + jnp.log(total)

    def attend(slot, beside):
        vt = jnp.concatenate([t_s[slot, 2].T, jnp.ones((16, t), bf16)], axis=0)
        top = score(slot, 0)
        for i in range(n):
            following = score(slot, i + 1) if i + 1 < n else None
            weigh(i, vt, top)
            beside(i)
            top = following

    slot = step % 2

    @pl.when(step == 0)
    def _():
        def pre(r, _):
            here = rows_of(r, STRIP)
            x = x_ref[here, :].astype(f32)
            a_s[here, :] = (x * inv_rms(x)).astype(bf16)
            return _

        loop(t // STRIP, pre)
        for i in range(n):
            project(0, i)

    @pl.when((step > 0) & (step < last))
    def _():
        attend(1 - slot, functools.partial(project, slot))

    @pl.when(step == last)
    def _():
        attend(1 - slot, lambda i: None)

        def row(r, _):
            here = rows_of(r, 512)
            o = jnp.concatenate([o_s[i, here, :] for i in range(o_s.shape[0])], axis=1)
            h_ref[here, :] = (x_ref[here, :].astype(f32) + dot(o, wo_ref[...]).astype(bf16).astype(f32)).astype(bf16)
            return _

        loop(t // 512, row)


def heads(x, wq, wk, wv, wo, cos, sin, layer, blk=512):
    t, d = x.shape
    number = d // HEAD
    now, before = lambda s: jnp.minimum(s, number - 1), lambda s: jnp.maximum(s - 1, 0)
    w = pl.BlockSpec((None, d, HEAD), lambda s: (layer, 0, now(s)))
    mine = pl.BlockSpec((t, HEAD), lambda s: (0, now(s)))
    return pl.pallas_call(
        functools.partial(_heads, blk=blk, scale=SCALE), grid=(number + 1,),
        in_specs=[whole(t, d), w, w, w, pl.BlockSpec((None, d, d), lambda s: (layer, 0, 0), pipeline_mode=ONE), whole(t, HEAD // 2), whole(t, HEAD // 2)],
        out_specs=[mine, mine, mine, pl.BlockSpec((t, HEAD), lambda s: (0, before(s))), pl.BlockSpec((1, 1, t), lambda s: (before(s), 0, 0)), whole(t, d)],
        out_shape=[jax.ShapeDtypeStruct((t, d), bf16)] * 4 + [jax.ShapeDtypeStruct((number, 1, t), f32), jax.ShapeDtypeStruct((t, d), bf16)],
        scratch_shapes=[pltpu.VMEM((t, d), bf16), pltpu.VMEM((2, 3, t, HEAD), bf16), pltpu.VMEM((number, t, HEAD), bf16),
                        pltpu.VMEM((2, t, blk), f32), pltpu.VMEM((t, blk), bf16)],
        compiler_params=params(), cost_estimate=cost(8 * t * d * d + 4 * t * t * d), name="heads",
    )(x, wq, wk, wv, wo, cos, sin)


def _mlp(h_ref, wg_ref, wu_ref, wd_ref, y_ref, gate_ref, up_ref, b_s, acc_s, *, tm):
    j = pl.program_id(0)
    t = h_ref.shape[0]

    @pl.when(j == 0)
    def _():
        def pre(r, _):
            here = rows_of(r, STRIP)
            h = h_ref[here, :].astype(f32)
            b_s[here, :] = (h * inv_rms(h)).astype(bf16)
            acc_s[here, :] = jnp.zeros((STRIP, acc_s.shape[1]), f32)
            return _

        loop(t // STRIP, pre)

    def row(r, _):
        here = rows_of(r, tm)
        b = b_s[here, :]
        gate, up = dot(b, wg_ref[...]), dot(b, wu_ref[...])
        gate_ref[here, :], up_ref[here, :] = gate, up
        act = (gate * (half_tanh(gate) + 0.5) * up).astype(bf16)
        acc_s[here, :] += dot(act, wd_ref[...])
        return _

    loop(t // tm, row)

    @pl.when(j == pl.num_programs(0) - 1)
    def _():
        def post(r, _):
            here = rows_of(r, STRIP)
            y_ref[here, :] = (h_ref[here, :].astype(f32) + acc_s[here, :].astype(bf16).astype(f32)).astype(bf16)
            return _

        loop(t // STRIP, post)


def mlp(h, wg, wu, wd, layer, tf=512, tm=1024):
    t, d = h.shape
    ff = wg.shape[2]
    full = whole(t, d)
    cols = pl.BlockSpec((None, d, tf), lambda j: (layer, 0, j))
    return pl.pallas_call(
        functools.partial(_mlp, tm=tm), grid=(ff // tf,),
        in_specs=[full, cols, cols, pl.BlockSpec((None, tf, d), lambda j: (layer, j, 0))],
        out_specs=[full, pl.BlockSpec((None, t, tf), lambda j: (j, 0, 0)), pl.BlockSpec((None, t, tf), lambda j: (j, 0, 0))],
        out_shape=[jax.ShapeDtypeStruct((t, d), bf16)] + [jax.ShapeDtypeStruct((ff // tf, t, tf), f32)] * 2,
        scratch_shapes=[pltpu.VMEM((t, d), bf16), pltpu.VMEM((t, d), f32)],
        compiler_params=params(), cost_estimate=cost(6 * t * d * ff), name="mlp",
    )(h, wg, wu, wd)


MESH = pl.DeviceIdType.MESH


def place():
    i = lax.axis_index("dp")
    c, y, x = i % 2, i // 2 % 2, i // 4
    return (c, y, x), (i + 1 - 2 * c, i + 2 - 4 * y, i + 4 - 8 * x)


def meet(others):
    barrier = pltpu.get_barrier_semaphore()
    for other in others:
        pl.semaphore_signal(barrier, device_id={"dp": other}, device_id_type=MESH)
    pl.semaphore_wait(barrier, len(others))


def everyone():
    return [(lax.axis_index("dp") + k) % 8 for k in range(1, 8)]


def sending(src, dst, send, recv, to):
    return pltpu.make_async_remote_copy(src, dst, send, recv, device_id={"dp": to}, device_id_type=MESH)


class Scatter:
    def __init__(self, g, r0, p1, r1, p2, r2, s0, v0, s1, v1, s2, v2, more=()):
        self.terms = [g.at[m] for m in range(g.shape[0])] + list(more)
        self.g, self.r0, self.p1, self.r1, self.p2, self.r2 = g, r0, p1, r1, p2, r2
        self.s0, self.v0, self.s1, self.v1, self.s2, self.v2 = s0, v0, s1, v1, s2, v2
        self.rows, self.cols = g.shape[1:]
        self.at, self.to = place()

    @staticmethod
    def scratch(n, rows, cols, slots=1, more=0):
        mine, n = n, n + more
        half, eighth, last = rows // 2, rows // 8, rows // 16
        shapes = [(mine, rows), (slots, n, half), (n, half), (n, 2, eighth), (n, 2, eighth), (n, 2, last)]
        one, two = pltpu.SemaphoreType.DMA((slots, n)), pltpu.SemaphoreType.DMA((n, 2))
        return [pltpu.VMEM((*shape, cols), bf16) for shape in shapes] + [one, one] + [two] * 4

    def _first(self, m, slot):
        rows = rows_of(1 - self.at[0], self.rows // 2)
        return sending(self.terms[m].at[rows, :], self.r0.at[slot, m], self.s0.at[slot, m], self.v0.at[slot, m], self.to[0])

    def _second(self, m):
        n = self.rows // 8
        (_, y, x), (_, py, px) = self.at, self.to
        return [sending(self.p1.at[m, rows_of(2 * k + 1 - own, n), :], self.r1.at[m, k], self.s1.at[m, k], self.v1.at[m, k], to)
                for k, (own, to) in enumerate(((x, px), (y, py)))]

    def _third(self, m):
        n = self.rows // 16
        (_, y, x), (_, py, px) = self.at, self.to
        return [sending(self.p2.at[m, k, rows_of(1 - own, n), :], self.r2.at[m, k], self.s2.at[m, k], self.v2.at[m, k], to)
                for k, (own, to) in enumerate(((y, py), (x, px)))]

    def start(self, m, slot=0):
        self._first(m, slot).start()

    def cross_one(self, m, slot=0):
        half, step = self.rows // 2, 128
        self._first(m, slot).wait()

        def add(i, _):
            here = rows_of(i, step)
            own = self.terms[m][rows_of(self.at[0] * (half // step) + i, step), :]
            self.p1[m, here, :] = (own.astype(f32) + self.r0[slot, m, here, :].astype(f32)).astype(bf16)
            return _

        loop(half // step, add)
        for copy in self._second(m):
            copy.start()

    def cross_two(self, m):
        _, y, x = self.at
        for copy in self._second(m):
            copy.wait()
        for k, own in enumerate((x, y)):
            term = self.p1[m, rows_of(2 * k + own, self.rows // 8), :]
            self.p2[m, k] = (term.astype(f32) + self.r1[m, k].astype(f32)).astype(bf16)
        for copy in self._third(m):
            copy.start()

    def finish(self, m, out, squares):
        _, y, x = self.at
        n = self.rows // 16
        for copy in self._third(m):
            copy.wait()
        for k, own in enumerate((y, x)):
            term = self.p2[m, k, rows_of(own, n), :]
            total = (term.astype(f32) + self.r2[m, k].astype(f32)).astype(bf16)
            out[k] = total
            wide = total.astype(f32)
            squares[...] += jnp.sum((wide * wide).reshape(n // 8, 8, self.cols // 128, 128), axis=(0, 2))


def sum_of_all(mine, got, send, recv):
    me = lax.axis_index("dp")
    copies = [sending(mine, got.at[me], send.at[k], recv.at[k], to) for k, to in enumerate(everyone())]
    for copy in copies:
        copy.start()
    got[me] = mine[...]
    for copy in copies:
        copy.wait_send()
    for k, to in enumerate(everyone()):
        sending(mine, got.at[(me + 7 - k) % 8], send.at[k], recv.at[k], to).wait_recv()
    return sum(got[k] for k in range(8))


def _mlp_back(h_ref, dy_ref, wg_ref, wu_ref, wd_ref, *refs, tm, saved):
    if saved:
        gate_ref, up_ref, more_ref, out_ref, own_ref, sq_ref, dh_ref, gu_s, gu_sem, acc_s, bt_s, at_s, dg_s, du_s, *comm = refs
    else:
        out_ref, sq_ref, dh_ref, b_s, acc_s, bt_s, at_s, dg_s, du_s, *comm = refs
    j, last = pl.program_id(0), pl.num_programs(0) - 1
    t, d = h_ref.shape
    tf = wg_ref.shape[1]
    steps = t // tm
    sums = Scatter(*comm, [more_ref.at[0]] if saved else [])
    done = lambda m, tile: sums.finish(m, out_ref.at[tile, m], sq_ref)

    def fetch(tile, r):
        return [pltpu.make_async_copy(ref.at[tile, rows_of(r, tm), :], gu_s.at[r % 2, i], gu_sem.at[r % 2, i])
                for i, ref in enumerate((gate_ref, up_ref))]

    @pl.when(j == 0)
    def _():
        if saved:
            for copy in fetch(0, 0):
                copy.start()
        meet(place()[1])
        sq_ref[...] = jnp.zeros_like(sq_ref)

        def pre(r, _):
            here = rows_of(r, STRIP)
            h = h_ref[here, :].astype(f32)
            b = (h * inv_rms(h)).astype(bf16)
            if not saved:
                b_s[here, :] = b
            bt_s[:, here] = b.T
            acc_s[here, :] = jnp.zeros((STRIP, d), f32)
            return _

        loop(t // STRIP, pre)

    if saved:
        sums.start(3)

    def row(r, _):
        here = rows_of(r, tm)
        if saved:
            tile, following = j + (r + 1) // steps, (r + 1) % steps

            @pl.when(tile <= last)
            def _():
                for copy in fetch(tile, following):
                    copy.start()

            for copy in fetch(j, r):
                copy.wait()
            gate, up = gu_s[r % 2, 0], gu_s[r % 2, 1]
        else:
            b = b_s[here, :]
            gate, up = dot(b, wg_ref[...]), dot(b, wu_ref[...])
        da = dot(dy_ref[here, :], wd_ref[...], 1, 1).astype(bf16).astype(f32)
        at = half_tanh(gate)
        s = at + 0.5
        silu = gate * s
        at_s[:, here] = (silu * up).astype(bf16).T
        du = (da * silu).astype(bf16)
        dg = (da * up * (s + silu * (0.5 - at))).astype(bf16)
        du_s[here, :] = du
        dg_s[here, :] = dg
        acc_s[here, :] += dot(dg, wg_ref[...], 1, 1) + dot(du, wu_ref[...], 1, 1)

        @pl.when((j > 0) & (r == 0))
        def _():
            sums.cross_one(2)
            sums.cross_two(0)

        if saved:

            @pl.when(r == 1)
            def _():
                @pl.when(j > 0)
                def _():
                    sums.finish(3, own_ref.at[j - 1], sq_ref)

                sums.cross_one(3)

        @pl.when((j > 0) & (r == 2))
        def _():
            sums.cross_two(1)

        return _

    loop(steps, row)

    @pl.when(j > 0)
    def _():
        sums.cross_two(2)

    for m, term in enumerate((dg_s, du_s)):
        sums.g[m] = dot(bt_s[...], term[...]).astype(bf16)

        @pl.when(j > 0)
        def _():
            done(m, j - 1)
            if m:
                done(2, j - 1)

        if m:
            if saved:
                sums.cross_two(3)
            sums.cross_one(0)
        sums.start(m)

    for k in range(d // tf):
        sums.g[2, k * tf : (k + 1) * tf, :] = dot(at_s[...], dy_ref[:, k * tf : (k + 1) * tf]).astype(bf16)
    sums.cross_one(1)
    sums.start(2)

    @pl.when(j == last)
    def _():
        def post(r, _):
            here = rows_of(r, STRIP)
            by_b = acc_s[here, :].astype(bf16).astype(f32)
            dh_ref[here, :] = (dy_ref[here, :].astype(f32) + norm_back(h_ref[here, :].astype(f32), by_b)).astype(bf16)
            return _

        loop(t // STRIP, post)
        sums.cross_one(2)
        sums.cross_two(0)
        sums.cross_two(1)
        done(0, j)
        if saved:
            sums.finish(3, own_ref.at[j], sq_ref)
        sums.cross_two(2)
        done(1, j)
        done(2, j)


def mlp_back(h, dy, wg, wu, wd, layer, saved=(), tf=512, tm=512):
    t, d = h.shape
    ff = wg.shape[2]
    tiles = ff // tf
    full = whole(t, d)
    cols = pl.BlockSpec((None, d, tf), lambda j: (layer, 0, j))
    own, more = (tiles, 3, 2, d // 16, tf), (tiles, 2, d // 16, tf)
    results = [own, more] if saved else [own]
    given = [pl.BlockSpec(memory_space=pl.ANY)] * 2 + [pl.BlockSpec((1, d, tf), lambda j: (j, 0, 0))] if saved else []
    first = [pltpu.VMEM((2, 2, tm, tf), f32), pltpu.SemaphoreType.DMA((2, 2))] if saved else [pltpu.VMEM((t, d), bf16)]
    return pl.pallas_call(
        functools.partial(_mlp_back, tm=tm, saved=bool(saved)), grid=(tiles,),
        in_specs=[full, full, cols, cols, pl.BlockSpec((None, tf, d), lambda j: (layer, j, 0))] + given,
        out_specs=[whole(*shape) for shape in results] + [STAT, full],
        out_shape=[jax.ShapeDtypeStruct(shape, bf16) for shape in results] + [jax.ShapeDtypeStruct((8, 128), f32), jax.ShapeDtypeStruct((t, d), bf16)],
        scratch_shapes=first + [pltpu.VMEM((t, d), f32)] + [pltpu.VMEM(shape, bf16) for shape in ((d, t), (tf, t), (t, tf), (t, tf))] + Scatter.scratch(3, d, tf, more=int(bool(saved))),
        compiler_params=params(collective_id=layer, has_side_effects=True), cost_estimate=cost(16 * t * d * ff),
    )(h, dy, wg, wu, wd, *saved)


def _attn_back(x_ref, dh_ref, q_ref, k_ref, v_ref, o_ref, lse_ref, wq_ref, wk_ref, wv_ref, wo_ref, cos_ref, sin_ref, *refs, blk, scale, inner):
    if inner:
        grad_ref, dx_ref, at_s, acc_s, do_s, delta_s, p_s, ds_s, dqt_s, dk_s, dv_s, g_s = refs
    else:
        one_ref, two_ref, out_ref, all_ref, at_s, do_s, delta_s, p_s, ds_s, dqt_s, dk_s, dv_s, g_s, sq_ref, tot_s, got_s, *flags = refs
        sums = Scatter(*flags[2:])
        grad_ref = sums.g
    head, last = pl.program_id(0), pl.num_programs(0) - 1
    t, d = x_ref.shape
    blocks, slot = range(2), head % 2
    n = t // blk
    e = scale * LOG2E

    @pl.when(head == 0)
    def _():
        if not inner:
            meet(everyone())
            sq_ref[...] = jnp.zeros_like(sq_ref)

        def pre(r, _):
            here = rows_of(r, STRIP)
            h = x_ref[here, :].astype(f32)
            at_s[:, here] = (h * inv_rms(h)).astype(bf16).T
            if inner:
                acc_s[here, :] = jnp.zeros((STRIP, d), f32)
            return _

        loop(t // STRIP, pre)

    for i in range(n):
        here = pl.ds(i * blk, blk)
        do = dot(dh_ref[here, :], wo_ref[...], 1, 1).astype(bf16)
        do_s[here, :] = do
        delta = jnp.sum(do.astype(f32) * o_ref[here, :].astype(f32), -1, keepdims=True)
        delta_s[:, here] = jnp.broadcast_to(delta, (blk, 128)).T[:8, :]

    if not inner:

        @pl.when(head > 0)
        def _():
            for m in blocks:
                sums.cross_one(1 - m, 1 - slot)

    dqt_s[...] = jnp.zeros_like(dqt_s)
    for j in range(n):
        kj, vj = k_ref[j * blk : (j + 1) * blk, :], v_ref[j * blk : (j + 1) * blk, :]
        for i in range(j, n):
            cols = pl.ds(i * blk, blk)
            s = dot(kj, q_ref[cols, :], 1, 1)
            dp = dot(vj, do_s[cols, :], 1, 1)
            p = jnp.exp2(s * e - lse_ref[0, :, cols] * LOG2E)
            if i == j:
                gap = lax.broadcasted_iota(jnp.int32, (blk, blk), 1) - lax.broadcasted_iota(jnp.int32, (blk, blk), 0)
                p = jnp.where(gap >= 0, p, 0.0)
            p_s[:, cols] = p.astype(bf16)
            ds_s[:, cols] = (p * (dp - delta_s[0:1, cols])).astype(bf16)
        seen = slice(j * blk, t)
        dv_s[j * blk : (j + 1) * blk, :] = dot(p_s[:, seen], do_s[seen, :]).astype(bf16)
        dk_s[j * blk : (j + 1) * blk, :] = dot(ds_s[:, seen], q_ref[seen, :])
        dqt_s[:, seen] += dot(kj.T, ds_s[:, seen])

    if not inner:

        @pl.when(head > 0)
        def _():
            for m in blocks:
                sums.cross_two(m)

    ot = o_ref[...].T
    for k in range(d // HEAD):
        grad_ref[1, k * HEAD : (k + 1) * HEAD, HEAD:] = dot(ot, dh_ref[:, k * HEAD : (k + 1) * HEAD]).astype(bf16)
    grad_ref[1, :, :HEAD] = dot(at_s[...], dv_s[...]).astype(bf16)
    if not inner:
        sums.start(1, slot)

    half = HEAD // 2
    for i in range(n):
        here = pl.ds(i * blk, blk)
        cos, sin = cos_ref[here, :], sin_ref[here, :]
        for which, g in ((0, dqt_s[:, here].T), (1, dk_s[here, :])):
            g = (g * scale).astype(bf16).astype(f32)
            a, b = g[:, :half], g[:, half:]
            g_s[here, which * HEAD : which * HEAD + half] = (a * cos + b * sin).astype(bf16)
            g_s[here, which * HEAD + half : (which + 1) * HEAD] = (b * cos - a * sin).astype(bf16)

    grad_ref[0] = dot(at_s[...], g_s[...]).astype(bf16)
    if inner:
        for i in range(n):
            here = pl.ds(i * blk, blk)
            acc_s[here, :] += (dot(g_s[here, :HEAD], wq_ref[...], 1, 1) + dot(g_s[here, HEAD:], wk_ref[...], 1, 1)
                               + dot(dv_s[here, :], wv_ref[...], 1, 1))

        @pl.when(head == last)
        def _():
            def post(r, _):
                here = rows_of(r, STRIP)
                by_a = acc_s[here, :].astype(bf16).astype(f32)
                dx_ref[here, :] = (dh_ref[here, :].astype(f32) + norm_back(x_ref[here, :].astype(f32), by_a)).astype(bf16)
                return _

            loop(t // STRIP, post)

        return

    @pl.when(head > 0)
    def _():
        for m in blocks:
            sums.finish(m, out_ref.at[head - 1, m], sq_ref)

    sums.start(0, slot)

    @pl.when(head == last)
    def _():
        for m in blocks:
            sums.cross_one(1 - m, slot)
        for m in blocks:
            sums.cross_two(1 - m)
        for m in blocks:
            sums.finish(1 - m, out_ref.at[head, 1 - m], sq_ref)
        tot_s[...] = sq_ref[...] + one_ref[...] + two_ref[...]
        all_ref[...] = sum_of_all(tot_s, got_s, *flags[:2])


def attn_back(x, dh, q, k, v, o, lse, wq, wk, wv, wo, cos, sin, layer, squares, blk=512):
    t, d = x.shape
    heads = d // HEAD
    inner = squares is None
    full = whole(t, d)
    one = pl.BlockSpec((t, HEAD), lambda h: (0, h))
    cols = pl.BlockSpec((None, d, HEAD), lambda h: (layer, 0, h))
    tab = whole(t, HEAD // 2)
    own, stat = (heads, 2, 2, d // 16, 2 * HEAD), (8, 128)
    flags = pltpu.SemaphoreType.DMA((7,))
    heads_first = [pltpu.VMEM((t, HEAD), bf16), pltpu.VMEM((8, t), f32), pltpu.VMEM((blk, t), bf16), pltpu.VMEM((blk, t), bf16),
                   pltpu.VMEM((HEAD, t), f32), pltpu.VMEM((t, HEAD), f32), pltpu.VMEM((t, HEAD), bf16), pltpu.VMEM((t, 2 * HEAD), bf16)]
    if inner:
        more = []
        outs = [pl.BlockSpec((2, d, 2 * HEAD), lambda h: (h, 0, 0)), full]
        shapes = [jax.ShapeDtypeStruct((2 * heads, d, 2 * HEAD), bf16), jax.ShapeDtypeStruct((t, d), bf16)]
        scratch = [pltpu.VMEM((d, t), bf16), pltpu.VMEM((t, d), f32)] + heads_first
        comm = {}
    else:
        more = [STAT] * len(squares)
        outs = [whole(*own), STAT]
        shapes = [jax.ShapeDtypeStruct(own, bf16), jax.ShapeDtypeStruct(stat, f32)]
        scratch = [pltpu.VMEM((d, t), bf16)] + heads_first + [pltpu.VMEM(stat, f32), pltpu.VMEM(stat, f32), pltpu.VMEM((8, *stat), f32)]
        scratch += [flags, flags] + Scatter.scratch(2, d, 2 * HEAD, 2)
        comm = {"collective_id": 2, "has_side_effects": True}
    return pl.pallas_call(
        functools.partial(_attn_back, blk=blk, scale=SCALE, inner=inner), grid=(heads,),
        in_specs=[full, full, one, one, one, one, pl.BlockSpec((1, 1, t), lambda h: (h, 0, 0)), cols, cols, cols,
                  pl.BlockSpec((None, HEAD, d), lambda h: (layer, h, 0)), tab, tab] + more,
        out_specs=outs, out_shape=shapes, scratch_shapes=scratch,
        compiler_params=params(**comm), cost_estimate=cost(22 * t * d * d + 8 * t * t * d),
    )(x, dh, q, k, v, o, lse, wq, wk, wv, wo, cos, sin, *(squares or ()))


def tables(t):
    half, lane = HEAD // 2, 128
    by = THETA ** (-jnp.arange(half, dtype=f32) / half)
    high = (jnp.arange(t // lane, dtype=f32) * lane)[:, None, None] * by
    low = jnp.arange(lane, dtype=f32)[:, None] * by
    (ch, sh), (cl, sl) = lax.optimization_barrier(((jnp.cos(high), jnp.sin(high)), (jnp.cos(low), jnp.sin(low))))
    return (ch * cl - sh * sl).reshape(t, half), (sh * cl + ch * sl).reshape(t, half)


def owner(half, late, s):
    hi, lo = s // 2, s % 2
    x, y = hi + (lo - hi) * late, lo + (hi - lo) * late
    return x * 4 + y * 2 + half


def flat(g, which, cols):
    _, blocks, _, _, n, wide = g.shape
    each = wide // cols
    return pl.BlockSpec((1, blocks, 1, 1, n, cols),
                        lambda r: (owner(r // 8, r // 4 % 2, r % 4), 0, which // each, r // 4 % 2, 0, which % each))


def piece(g, which, cols, index):
    each = g.shape[5] // cols

    def at(r):
        half, late, s, block = index(r)
        return owner(half, late, s), block, which // each, late, 0, which % each

    return pl.BlockSpec((1, 1, 1, 1, g.shape[4], cols), at)


def update(refs, which, at, g, factor):
    n = len(refs) // 6
    w_ref, m_ref, v_ref, w_out, m_out, v_out = (refs[kind * n + which] for kind in range(6))
    g = g.astype(f32) * factor
    m = 0.9 * m_ref[at] + 0.1 * g
    v = 0.95 * v_ref[at] + 0.05 * g * g
    w = w_ref[at].astype(f32)
    w_out[at] = (w - 0.02 * (m * lax.rsqrt(v + 1e-8) + 0.1 * w)).astype(bf16)
    m_out[at] = m
    v_out[at] = v


def _adam(sq_ref, *refs, count, flats, pieces, arrays, cols):
    factor = jnp.minimum(1.0, 0.5 * lax.rsqrt(jnp.sum(sq_ref[...]) / count + 1e-30))
    n_flat, n_given = flats, flats + len(pieces)
    state = refs[n_given : n_given + arrays] + refs[len(refs) - arrays :]
    for which in range(n_flat):
        for k in range(refs[which].shape[1]):
            update(state, which, (slice(None), slice(k * cols, (k + 1) * cols)), refs[which][0, k, 0, 0], factor)
    for ref, (row, col) in zip(refs[n_flat:n_given], pieces):
        rows = ref.shape[4]
        at = slice(row * rows, (row + 1) * rows), slice(col * cols, (col + 1) * cols)
        update(state, n_flat, at, ref[0, 0, 0, 0], factor)


def adam(squares, g, arrays, layer, before, count):
    n = g.shape[4]
    d = arrays[0].shape[1]
    flats = len(arrays) // 3 - 1
    cols = g.shape[2] * g.shape[5] // (flats + 1)
    tall = arrays[flats].shape[1] // (d // n)
    across = d // cols
    if tall == n:
        places = [(0, k) for k in range(across)]
        spec = [piece(g, flats, cols, lambda r, k=k: (k // 2, k % 2, r % 4, r // 4)) for k in range(across)]
    else:
        places = [(s, k) for s in range(tall // n) for k in range(across)]
        spec = [piece(g, flats, cols, lambda r, s=s, k=k: (k, r % 2, s, r // 2)) for s, k in places]
    kinds = [pl.BlockSpec((None, n, a.shape[2]), lambda r: (layer, r, 0)) for a in arrays[:flats]]
    kinds = (kinds + [pl.BlockSpec((None, tall, d), lambda r: (layer, r, 0))]) * 3
    given = [squares] + [g] * (flats + len(places)) + list(arrays)
    specs = [STAT] + [flat(g, which, cols) for which in range(flats)] + spec + kinds
    aliases = {}
    if before is not None:
        aliases = {len(given) + i: i for i in range(len(arrays))}
        given += list(before)
        specs += [pl.BlockSpec(memory_space=pl.ANY)] * len(arrays)
    return pl.pallas_call(
        functools.partial(_adam, count=count, flats=flats, pieces=places, arrays=len(arrays), cols=cols), grid=(d // n,),
        in_specs=specs, out_specs=kinds, out_shape=[jax.ShapeDtypeStruct(a.shape, a.dtype) for a in arrays],
        input_output_aliases=aliases, compiler_params=params(), cost_estimate=cost(4000 * arrays[0].size), name="adam",
    )(*given)


def solution(mesh):
    def step(x, dy, *arrays):
        weights, m, v = (arrays[i : i + 7] for i in (0, 7, 14))
        wq, wk, wv, wo, wg, wu, wd = weights
        cos, sin = tables(x.shape[1])
        layers = wq.shape[0]
        h, kept = x[0], []
        for n in range(layers):
            q, k, val, o, lse, mid = heads(h, wq, wk, wv, wo, cos, sin, n)
            kept.append((h, q, k, val, o, lse, mid))
            if n < layers - 1:
                h, *saved = mlp(mid, wg, wu, wd, n)
        parts = []

        def gather(n, a, b, own):
            parts.append((n, a, b, lax.all_gather(own, "dp")))

        h, q, k, val, o, lse, mid = kept[1]
        own, square_1, dh = mlp_back(mid, dy[0], wg, wu, wd, 1)
        gather(1, 4, 7, own)
        terms, by_h = attn_back(h, dh, q, k, val, o, lse, wq, wk, wv, wo, cos, sin, 1, None)
        h, q, k, val, o, lse, mid = kept[0]
        own, more, square_0, dh = mlp_back(mid, by_h, wg, wu, wd, 0, (*saved, terms))
        gather(1, 0, 4, more.reshape(-1, 2, *more.shape[1:]))
        gather(0, 4, 7, own)
        own, total = attn_back(h, dh, q, k, val, o, lse, wq, wk, wv, wo, cos, sin, 0, (square_1, square_0))
        gather(0, 0, 4, own)
        count = sum(w.size for w in weights)
        new = {0: None, 4: None}
        for n, a, b, g in parts:
            new[a] = adam(total, g, (*weights[a:b], *m[a:b], *v[a:b]), n, new[a], count)
        return tuple(one for i in range(3) for a, size in ((0, 4), (4, 3)) for one in new[a][size * i : size * (i + 1)])

    states, all_of = P(("rep", "dp"), None, None), P(None, None, None)
    return jax.shard_map(
        step, mesh=mesh, in_specs=(states, states) + (all_of,) * 21, out_specs=(P("rep", None, None),) * 21, check_vma=False,
    )
```

```python
import functools

import jax
import jax.numpy as jnp
from jax import lax
from jax.experimental import pallas as pl
from jax.experimental.pallas import tpu as pltpu
from jax.sharding import PartitionSpec as P


HEAD = 256
STRIP = 256
THETA = 10000
EPS = 1e-6
LOG2E = 1.4426950408889634
HIDDEN = -2e30
SCALE = HEAD**-0.5
f32, bf16 = jnp.float32, jnp.bfloat16
VMEM = 67_043_328
ONE = pl.Buffered(1)
STAT = pl.BlockSpec((8, 128), lambda *_: (0, 0))


def dot(a, b, ca=1, cb=0):
    return lax.dot_general(a, b, (((ca,), (cb,)), ((), ())), preferred_element_type=f32)


def loop(n, body):
    lax.fori_loop(0, n, body, None)


def whole(*shape):
    return pl.BlockSpec(shape, lambda *_: (0,) * len(shape), pipeline_mode=ONE)


def rows_of(i, n):
    return pl.ds(pl.multiple_of(i * n, n), n)


def inv_rms(h):
    return lax.rsqrt(jnp.mean(h * h, -1, keepdims=True) + EPS)


def half_tanh(x):
    return 0.5 * jnp.tanh(0.5 * x)


def norm_back(h, by_out):
    scale = inv_rms(h)
    return scale * (by_out - h * (scale * scale * jnp.mean(by_out * h, -1, keepdims=True)))


def cost(flops):
    return pl.CostEstimate(flops=flops, transcendentals=0, bytes_accessed=0)


def params(**more):
    return pltpu.CompilerParams(dimension_semantics=("arbitrary",), vmem_limit_bytes=VMEM, **more)


def _heads(x_ref, wq_ref, wk_ref, wv_ref, wo_ref, cos_ref, sin_ref, q_ref, k_ref, v_ref, o_ref, lse_ref, h_ref, a_s, t_s, o_s, s_s, p_s, *, blk, scale):
    step, last = pl.program_id(0), pl.num_programs(0) - 1
    t = x_ref.shape[0]
    n, half, e = t // blk, HEAD // 2, scale * LOG2E
    rows = [slice(i * blk, (i + 1) * blk) for i in range(n)]

    def project(slot, i):
        a, cos, sin = a_s[rows[i], :], cos_ref[rows[i], :], sin_ref[rows[i], :]
        for which, (w_ref, out_ref) in enumerate(((wq_ref, q_ref), (wk_ref, k_ref), (wv_ref, v_ref))):
            r = dot(a, w_ref[...]).astype(bf16)
            if which < 2:
                p, m = r[:, :half].astype(f32), r[:, half:].astype(f32)
                r = jnp.concatenate([p * cos - m * sin, m * cos + p * sin], axis=1).astype(bf16)
            out_ref[rows[i], :] = r
            t_s[slot, which, rows[i], :] = r

    def score(slot, i):
        q, top = t_s[slot, 0, rows[i], :], None
        for j in range(i + 1):
            s = dot(t_s[slot, 1, rows[j], :], q, 1, 1)
            if i == j:
                gap = lax.broadcasted_iota(jnp.int32, (blk, blk), 1) - lax.broadcasted_iota(jnp.int32, (blk, blk), 0)
                s = jnp.where(gap >= 0, s, HIDDEN)
            s_s[i % 2, rows[j], :] = s
            m = s.max(axis=0, keepdims=True)
            top = m if top is None else jnp.maximum(top, m)
        return top

    def weigh(i, vt, top):
        for j in range(i + 1):
            p_s[rows[j], :] = jnp.exp2((s_s[i % 2, rows[j], :] - top) * e).astype(bf16)
        seen = (i + 1) * blk
        mix = dot(vt[:, :seen], p_s[:seen, :])
        total = mix[HEAD : HEAD + 1, :]
        o = (mix[:HEAD, :] * (1 / total)).T.astype(bf16)
        o_ref[rows[i], :] = o
        o_s[step - 1, rows[i], :] = o
        lse_ref[0, :, rows[i]] = top * scale + jnp.log(total)

    def attend(slot, beside):
        vt = jnp.concatenate([t_s[slot, 2].T, jnp.ones((16, t), bf16)], axis=0)
        top = score(slot, 0)
        for i in range(n):
            following = score(slot, i + 1) if i + 1 < n else None
            weigh(i, vt, top)
            beside(i)
            top = following

    slot = step % 2

    @pl.when(step == 0)
    def _():
        def pre(r, _):
            here = rows_of(r, STRIP)
            x = x_ref[here, :].astype(f32)
            a_s[here, :] = (x * inv_rms(x)).astype(bf16)
            return _

        loop(t // STRIP, pre)
        for i in range(n):
            project(0, i)

    @pl.when((step > 0) & (step < last))
    def _():
        attend(1 - slot, functools.partial(project, slot))

    @pl.when(step == last)
    def _():
        attend(1 - slot, lambda i: None)

        def row(r, _):
            here = rows_of(r, 512)
            o = jnp.concatenate([o_s[i, here, :] for i in range(o_s.shape[0])], axis=1)
            h_ref[here, :] = (x_ref[here, :].astype(f32) + dot(o, wo_ref[...]).astype(bf16).astype(f32)).astype(bf16)
            return _

        loop(t // 512, row)


def heads(x, wq, wk, wv, wo, cos, sin, layer, blk=512):
    t, d = x.shape
    number = d // HEAD
    now, before = lambda s: jnp.minimum(s, number - 1), lambda s: jnp.maximum(s - 1, 0)
    w = pl.BlockSpec((None, d, HEAD), lambda s: (layer, 0, now(s)))
    mine = pl.BlockSpec((t, HEAD), lambda s: (0, now(s)))
    return pl.pallas_call(
        functools.partial(_heads, blk=blk, scale=SCALE), grid=(number + 1,),
        in_specs=[whole(t, d), w, w, w, pl.BlockSpec((None, d, d), lambda s: (layer, 0, 0), pipeline_mode=ONE), whole(t, HEAD // 2), whole(t, HEAD // 2)],
        out_specs=[mine, mine, mine, pl.BlockSpec((t, HEAD), lambda s: (0, before(s))), pl.BlockSpec((1, 1, t), lambda s: (before(s), 0, 0)), whole(t, d)],
        out_shape=[jax.ShapeDtypeStruct((t, d), bf16)] * 4 + [jax.ShapeDtypeStruct((number, 1, t), f32), jax.ShapeDtypeStruct((t, d), bf16)],
        scratch_shapes=[pltpu.VMEM((t, d), bf16), pltpu.VMEM((2, 3, t, HEAD), bf16), pltpu.VMEM((number, t, HEAD), bf16),
                        pltpu.VMEM((2, t, blk), f32), pltpu.VMEM((t, blk), bf16)],
        compiler_params=params(), cost_estimate=cost(8 * t * d * d + 4 * t * t * d), name="heads",
    )(x, wq, wk, wv, wo, cos, sin)


def _mlp(h_ref, wg_ref, wu_ref, wd_ref, y_ref, gate_ref, up_ref, b_s, acc_s, *, tm):
    j = pl.program_id(0)
    t = h_ref.shape[0]

    @pl.when(j == 0)
    def _():
        def pre(r, _):
            here = rows_of(r, STRIP)
            h = h_ref[here, :].astype(f32)
            b_s[here, :] = (h * inv_rms(h)).astype(bf16)
            acc_s[here, :] = jnp.zeros((STRIP, acc_s.shape[1]), f32)
            return _

        loop(t // STRIP, pre)

    def row(r, _):
        here = rows_of(r, tm)
        b = b_s[here, :]
        gate, up = dot(b, wg_ref[...]), dot(b, wu_ref[...])
        gate_ref[here, :], up_ref[here, :] = gate, up
        act = (gate * (half_tanh(gate) + 0.5) * up).astype(bf16)
        acc_s[here, :] += dot(act, wd_ref[...])
        return _

    loop(t // tm, row)

    @pl.when(j == pl.num_programs(0) - 1)
    def _():
        def post(r, _):
            here = rows_of(r, STRIP)
            y_ref[here, :] = (h_ref[here, :].astype(f32) + acc_s[here, :].astype(bf16).astype(f32)).astype(bf16)
            return _

        loop(t // STRIP, post)


def mlp(h, wg, wu, wd, layer, tf=512, tm=1024):
    t, d = h.shape
    ff = wg.shape[2]
    full = whole(t, d)
    cols = pl.BlockSpec((None, d, tf), lambda j: (layer, 0, j))
    return pl.pallas_call(
        functools.partial(_mlp, tm=tm), grid=(ff // tf,),
        in_specs=[full, cols, cols, pl.BlockSpec((None, tf, d), lambda j: (layer, j, 0))],
        out_specs=[full, pl.BlockSpec((None, t, tf), lambda j: (j, 0, 0)), pl.BlockSpec((None, t, tf), lambda j: (j, 0, 0))],
        out_shape=[jax.ShapeDtypeStruct((t, d), bf16)] + [jax.ShapeDtypeStruct((ff // tf, t, tf), f32)] * 2,
        scratch_shapes=[pltpu.VMEM((t, d), bf16), pltpu.VMEM((t, d), f32)],
        compiler_params=params(), cost_estimate=cost(6 * t * d * ff), name="mlp",
    )(h, wg, wu, wd)


MESH = pl.DeviceIdType.MESH
GROUP = 8


def place():
    i = lax.axis_index("dp")
    c, y, x = i % 2, i // 2 % 2, i // 4
    return (c, y, x), (i + 1 - 2 * c, i + 2 - 4 * y, i + 4 - 8 * x)


def meet(others):
    barrier = pltpu.get_barrier_semaphore()
    for other in others:
        pl.semaphore_signal(barrier, device_id={"dp": other}, device_id_type=MESH)
    pl.semaphore_wait(barrier, len(others))


def everyone():
    return [(lax.axis_index("dp") + k) % GROUP for k in range(1, GROUP)]


def sending(src, dst, send, recv, to):
    return pltpu.make_async_remote_copy(src, dst, send, recv, device_id={"dp": to}, device_id_type=MESH)


class Scatter:
    def __init__(self, g, r0, p1, r1, p2, r2, s0, v0, s1, v1, s2, v2, more=()):
        self.terms = [g.at[m] for m in range(g.shape[0])] + list(more)
        self.g, self.r0, self.p1, self.r1, self.p2, self.r2 = g, r0, p1, r1, p2, r2
        self.s0, self.v0, self.s1, self.v1, self.s2, self.v2 = s0, v0, s1, v1, s2, v2
        self.rows, self.cols = g.shape[1:]
        self.at, self.to = place()

    @staticmethod
    def scratch(n, rows, cols, slots=1, more=0):
        mine, n = n, n + more
        half, eighth, last = rows // 2, rows // 8, rows // 16
        shapes = [(mine, rows), (slots, n, half), (n, half), (n, 2, eighth), (n, 2, eighth), (n, 2, last)]
        one, two = pltpu.SemaphoreType.DMA((slots, n)), pltpu.SemaphoreType.DMA((n, 2))
        return [pltpu.VMEM((*shape, cols), bf16) for shape in shapes] + [one, one] + [two] * 4

    def _first(self, m, slot):
        rows = rows_of(1 - self.at[0], self.rows // 2)
        return sending(self.terms[m].at[rows, :], self.r0.at[slot, m], self.s0.at[slot, m], self.v0.at[slot, m], self.to[0])

    def _second(self, m):
        n = self.rows // 8
        (_, y, x), (_, py, px) = self.at, self.to
        return [sending(self.p1.at[m, rows_of(2 * k + 1 - own, n), :], self.r1.at[m, k], self.s1.at[m, k], self.v1.at[m, k], to)
                for k, (own, to) in enumerate(((x, px), (y, py)))]

    def _third(self, m):
        n = self.rows // 16
        (_, y, x), (_, py, px) = self.at, self.to
        return [sending(self.p2.at[m, k, rows_of(1 - own, n), :], self.r2.at[m, k], self.s2.at[m, k], self.v2.at[m, k], to)
                for k, (own, to) in enumerate(((y, py), (x, px)))]

    def start(self, m, slot=0):
        self._first(m, slot).start()

    def cross_one(self, m, slot=0):
        half, step = self.rows // 2, 128
        self._first(m, slot).wait()

        def add(i, _):
            here = rows_of(i, step)
            own = self.terms[m][rows_of(self.at[0] * (half // step) + i, step), :]
            self.p1[m, here, :] = (own.astype(f32) + self.r0[slot, m, here, :].astype(f32)).astype(bf16)
            return _

        loop(half // step, add)
        for copy in self._second(m):
            copy.start()

    def cross_two(self, m):
        _, y, x = self.at
        for copy in self._second(m):
            copy.wait()
        for k, own in enumerate((x, y)):
            term = self.p1[m, rows_of(2 * k + own, self.rows // 8), :]
            self.p2[m, k] = (term.astype(f32) + self.r1[m, k].astype(f32)).astype(bf16)
        for copy in self._third(m):
            copy.start()

    def finish(self, m, out, squares):
        _, y, x = self.at
        n = self.rows // 16
        for copy in self._third(m):
            copy.wait()
        for k, own in enumerate((y, x)):
            term = self.p2[m, k, rows_of(own, n), :]
            total = (term.astype(f32) + self.r2[m, k].astype(f32)).astype(bf16)
            out[k] = total
            wide = total.astype(f32)
            squares[...] += jnp.sum((wide * wide).reshape(n // 8, 8, self.cols // 128, 128), axis=(0, 2))


def sum_of_all(mine, got, send, recv):
    me = lax.axis_index("dp")
    copies = [sending(mine, got.at[me], send.at[k], recv.at[k], to) for k, to in enumerate(everyone())]
    for copy in copies:
        copy.start()
    got[me] = mine[...]
    for copy in copies:
        copy.wait_send()
    for k, to in enumerate(everyone()):
        sending(mine, got.at[(me + GROUP - 1 - k) % GROUP], send.at[k], recv.at[k], to).wait_recv()
    return sum(got[k] for k in range(GROUP))


def _mlp_back(h_ref, dy_ref, wg_ref, wu_ref, wd_ref, *refs, tm, saved):
    if saved:
        gate_ref, up_ref, more_ref, out_ref, own_ref, sq_ref, dh_ref, gu_s, gu_sem, acc_s, bt_s, at_s, dg_s, du_s, *comm = refs
    else:
        out_ref, sq_ref, dh_ref, b_s, acc_s, bt_s, at_s, dg_s, du_s, *comm = refs
    j, last = pl.program_id(0), pl.num_programs(0) - 1
    t, d = h_ref.shape
    tf = wg_ref.shape[1]
    steps = t // tm
    sums = Scatter(*comm, [more_ref.at[0]] if saved else [])
    done = lambda m, tile: sums.finish(m, out_ref.at[tile, m], sq_ref)

    def fetch(tile, r):
        return [pltpu.make_async_copy(ref.at[tile, rows_of(r, tm), :], gu_s.at[r % 2, i], gu_sem.at[r % 2, i])
                for i, ref in enumerate((gate_ref, up_ref))]

    @pl.when(j == 0)
    def _():
        if saved:
            for copy in fetch(0, 0):
                copy.start()
        meet(place()[1])
        sq_ref[...] = jnp.zeros_like(sq_ref)

        def pre(r, _):
            here = rows_of(r, STRIP)
            h = h_ref[here, :].astype(f32)
            b = (h * inv_rms(h)).astype(bf16)
            if not saved:
                b_s[here, :] = b
            bt_s[:, here] = b.T
            acc_s[here, :] = jnp.zeros((STRIP, d), f32)
            return _

        loop(t // STRIP, pre)

    if saved:
        sums.start(3)

    def back(r):
        here = rows_of(r, tm)
        acc_s[here, :] += dot(dg_s[here, :], wg_ref[...], 1, 1) + dot(du_s[here, :], wu_ref[...], 1, 1)

    def row(adding, r, _):
        here = rows_of(r, tm)
        if saved:
            tile, following = j + (r + 1) // steps, (r + 1) % steps

            @pl.when(tile <= last)
            def _():
                for copy in fetch(tile, following):
                    copy.start()

            for copy in fetch(j, r):
                copy.wait()
            gate, up = gu_s[r % 2, 0], gu_s[r % 2, 1]
        else:
            b = b_s[here, :]
            gate, up = dot(b, wg_ref[...]), dot(b, wu_ref[...])
        da = dot(dy_ref[here, :], wd_ref[...], 1, 1).astype(bf16).astype(f32)
        at = half_tanh(gate)
        s = at + 0.5
        silu = gate * s
        at_s[:, here] = (silu * up).astype(bf16).T
        du_s[here, :] = (da * silu).astype(bf16)
        dg_s[here, :] = (da * up * (s + silu * (0.5 - at))).astype(bf16)
        if adding:
            back(r)

        @pl.when((j > 0) & (r == 0))
        def _():
            sums.cross_one(2)
            sums.cross_two(0)

        if saved:

            @pl.when(r == 1)
            def _():
                @pl.when(j > 0)
                def _():
                    sums.finish(3, own_ref.at[j - 1], sq_ref)

                sums.cross_one(3)

        @pl.when((j > 0) & (r == 2))
        def _():
            sums.cross_two(1)

        return _

    if saved:
        loop(steps, functools.partial(row, True))
    else:

        @pl.when(j < last)
        def _():
            loop(steps, functools.partial(row, True))

        @pl.when(j == last)
        def _():
            loop(steps, functools.partial(row, False))

    @pl.when(j > 0)
    def _():
        sums.cross_two(2)

    for m, term in enumerate((dg_s, du_s)):
        sums.g[m] = dot(bt_s[...], term[...]).astype(bf16)

        @pl.when(j > 0)
        def _():
            done(m, j - 1)
            if m:
                done(2, j - 1)

        if m:
            if saved:
                sums.cross_two(3)
            sums.cross_one(0)
        sums.start(m)

    for k in range(d // tf):
        sums.g[2, k * tf : (k + 1) * tf, :] = dot(at_s[...], dy_ref[:, k * tf : (k + 1) * tf]).astype(bf16)
    sums.cross_one(1)
    sums.start(2)

    @pl.when(j == last)
    def _():
        def post(r, _):
            here = rows_of(r, STRIP)
            by_b = acc_s[here, :].astype(bf16).astype(f32)
            dh_ref[here, :] = (dy_ref[here, :].astype(f32) + norm_back(h_ref[here, :].astype(f32), by_b)).astype(bf16)
            return _

        def crossings():
            sums.cross_one(2)
            sums.cross_two(0)

        if not saved:
            for r in range(steps):
                back(r)
                if r == 1:
                    crossings()
        loop(t // STRIP, post)
        if saved:
            crossings()
        sums.cross_two(1)
        done(0, j)
        if saved:
            sums.finish(3, own_ref.at[j], sq_ref)
        sums.cross_two(2)
        done(1, j)
        done(2, j)


def mlp_back(h, dy, wg, wu, wd, layer, saved=(), tf=512, tm=512):
    t, d = h.shape
    ff = wg.shape[2]
    tiles = ff // tf
    full = whole(t, d)
    cols = pl.BlockSpec((None, d, tf), lambda j: (layer, 0, j))
    own, more = (tiles, 3, 2, d // 16, tf), (tiles, 2, d // 16, tf)
    results = [own, more] if saved else [own]
    given = [pl.BlockSpec(memory_space=pl.ANY)] * 2 + [pl.BlockSpec((1, d, tf), lambda j: (j, 0, 0))] if saved else []
    first = [pltpu.VMEM((2, 2, tm, tf), f32), pltpu.SemaphoreType.DMA((2, 2))] if saved else [pltpu.VMEM((t, d), bf16)]
    return pl.pallas_call(
        functools.partial(_mlp_back, tm=tm, saved=bool(saved)), grid=(tiles,),
        in_specs=[full, full, cols, cols, pl.BlockSpec((None, tf, d), lambda j: (layer, j, 0))] + given,
        out_specs=[whole(*shape) for shape in results] + [STAT, full],
        out_shape=[jax.ShapeDtypeStruct(shape, bf16) for shape in results] + [jax.ShapeDtypeStruct((8, 128), f32), jax.ShapeDtypeStruct((t, d), bf16)],
        scratch_shapes=first + [pltpu.VMEM((t, d), f32)] + [pltpu.VMEM(shape, bf16) for shape in ((d, t), (tf, t), (t, tf), (t, tf))] + Scatter.scratch(3, d, tf, more=int(bool(saved))),
        compiler_params=params(collective_id=layer, has_side_effects=True), cost_estimate=cost(16 * t * d * ff),
    )(h, dy, wg, wu, wd, *saved)


def _attn_back(x_ref, dh_ref, q_ref, k_ref, v_ref, o_ref, lse_ref, wq_ref, wk_ref, wv_ref, wo_ref, cos_ref, sin_ref, *refs, blk, scale, inner):
    if inner:
        grad_ref, dx_ref, at_s, acc_s, do_s, delta_s, p_s, ds_s, dqt_s, dk_s, dv_s, g_s = refs
    else:
        one_ref, two_ref, out_ref, all_ref, at_s, do_s, delta_s, p_s, ds_s, dqt_s, dk_s, dv_s, g_s, sq_ref, tot_s, got_s, *flags = refs
        sums = Scatter(*flags[2:])
        grad_ref = sums.g
    head, last = pl.program_id(0), pl.num_programs(0) - 1
    t, d = x_ref.shape
    blocks, slot = range(2), head % 2
    n = t // blk
    e = scale * LOG2E

    @pl.when(head == 0)
    def _():
        if not inner:
            meet(everyone())
            sq_ref[...] = jnp.zeros_like(sq_ref)

        def pre(r, _):
            here = rows_of(r, STRIP)
            h = x_ref[here, :].astype(f32)
            at_s[:, here] = (h * inv_rms(h)).astype(bf16).T
            if inner:
                acc_s[here, :] = jnp.zeros((STRIP, d), f32)
            return _

        loop(t // STRIP, pre)

    for i in range(n):
        here = pl.ds(i * blk, blk)
        do = dot(dh_ref[here, :], wo_ref[...], 1, 1).astype(bf16)
        do_s[here, :] = do
        delta = jnp.sum(do.astype(f32) * o_ref[here, :].astype(f32), -1, keepdims=True)
        delta_s[:, here] = jnp.broadcast_to(delta, (blk, 128)).T[:8, :]

    if not inner:

        @pl.when(head > 0)
        def _():
            for m in blocks:
                sums.cross_one(1 - m, 1 - slot)

    dqt_s[...] = jnp.zeros_like(dqt_s)
    for j in range(n):
        kj, vj = k_ref[j * blk : (j + 1) * blk, :], v_ref[j * blk : (j + 1) * blk, :]
        for i in range(j, n):
            cols = pl.ds(i * blk, blk)
            s = dot(kj, q_ref[cols, :], 1, 1)
            dp = dot(vj, do_s[cols, :], 1, 1)
            p = jnp.exp2(s * e - lse_ref[0, :, cols] * LOG2E)
            if i == j:
                gap = lax.broadcasted_iota(jnp.int32, (blk, blk), 1) - lax.broadcasted_iota(jnp.int32, (blk, blk), 0)
                p = jnp.where(gap >= 0, p, 0.0)
            p_s[:, cols] = p.astype(bf16)
            ds_s[:, cols] = (p * (dp - delta_s[0:1, cols])).astype(bf16)
        seen = slice(j * blk, t)
        dv_s[j * blk : (j + 1) * blk, :] = dot(p_s[:, seen], do_s[seen, :]).astype(bf16)
        dk_s[j * blk : (j + 1) * blk, :] = dot(ds_s[:, seen], q_ref[seen, :])
        dqt_s[:, seen] += dot(kj.T, ds_s[:, seen])

    if not inner:

        @pl.when(head > 0)
        def _():
            for m in blocks:
                sums.cross_two(m)

    ot = o_ref[...].T
    for k in range(d // HEAD):
        grad_ref[1, k * HEAD : (k + 1) * HEAD, HEAD:] = dot(ot, dh_ref[:, k * HEAD : (k + 1) * HEAD]).astype(bf16)
    grad_ref[1, :, :HEAD] = dot(at_s[...], dv_s[...]).astype(bf16)
    if not inner:
        sums.start(1, slot)

    half = HEAD // 2
    for i in range(n):
        here = pl.ds(i * blk, blk)
        cos, sin = cos_ref[here, :], sin_ref[here, :]
        for which, g in ((0, dqt_s[:, here].T), (1, dk_s[here, :])):
            g = (g * scale).astype(bf16).astype(f32)
            a, b = g[:, :half], g[:, half:]
            g_s[here, which * HEAD : which * HEAD + half] = (a * cos + b * sin).astype(bf16)
            g_s[here, which * HEAD + half : (which + 1) * HEAD] = (b * cos - a * sin).astype(bf16)

    grad_ref[0] = dot(at_s[...], g_s[...]).astype(bf16)
    if inner:
        for i in range(n):
            here = pl.ds(i * blk, blk)
            acc_s[here, :] += (dot(g_s[here, :HEAD], wq_ref[...], 1, 1) + dot(g_s[here, HEAD:], wk_ref[...], 1, 1)
                               + dot(dv_s[here, :], wv_ref[...], 1, 1))

        @pl.when(head == last)
        def _():
            def post(r, _):
                here = rows_of(r, STRIP)
                by_a = acc_s[here, :].astype(bf16).astype(f32)
                dx_ref[here, :] = (dh_ref[here, :].astype(f32) + norm_back(x_ref[here, :].astype(f32), by_a)).astype(bf16)
                return _

            loop(t // STRIP, post)

        return

    @pl.when(head > 0)
    def _():
        for m in blocks:
            sums.finish(m, out_ref.at[head - 1, m], sq_ref)

    sums.start(0, slot)

    @pl.when(head == last)
    def _():
        for m in blocks:
            sums.cross_one(1 - m, slot)
        for m in blocks:
            sums.cross_two(1 - m)
        for m in blocks:
            sums.finish(1 - m, out_ref.at[head, 1 - m], sq_ref)
        tot_s[...] = sq_ref[...] + one_ref[...] + two_ref[...]
        all_ref[...] = sum_of_all(tot_s, got_s, *flags[:2])


def attn_back(x, dh, q, k, v, o, lse, wq, wk, wv, wo, cos, sin, layer, squares, blk=512):
    t, d = x.shape
    heads = d // HEAD
    inner = squares is None
    full = whole(t, d)
    one = pl.BlockSpec((t, HEAD), lambda h: (0, h))
    cols = pl.BlockSpec((None, d, HEAD), lambda h: (layer, 0, h))
    tab = whole(t, HEAD // 2)
    own, stat = (heads, 2, 2, d // 16, 2 * HEAD), (8, 128)
    flags = pltpu.SemaphoreType.DMA((GROUP - 1,))
    heads_first = [pltpu.VMEM((t, HEAD), bf16), pltpu.VMEM((8, t), f32), pltpu.VMEM((blk, t), bf16), pltpu.VMEM((blk, t), bf16),
                   pltpu.VMEM((HEAD, t), f32), pltpu.VMEM((t, HEAD), f32), pltpu.VMEM((t, HEAD), bf16), pltpu.VMEM((t, 2 * HEAD), bf16)]
    if inner:
        more = []
        outs = [pl.BlockSpec((2, d, 2 * HEAD), lambda h: (h, 0, 0)), full]
        shapes = [jax.ShapeDtypeStruct((2 * heads, d, 2 * HEAD), bf16), jax.ShapeDtypeStruct((t, d), bf16)]
        scratch = [pltpu.VMEM((d, t), bf16), pltpu.VMEM((t, d), f32)] + heads_first
        comm = {}
    else:
        more = [STAT] * len(squares)
        outs = [whole(*own), STAT]
        shapes = [jax.ShapeDtypeStruct(own, bf16), jax.ShapeDtypeStruct(stat, f32)]
        scratch = [pltpu.VMEM((d, t), bf16)] + heads_first + [pltpu.VMEM(stat, f32), pltpu.VMEM(stat, f32), pltpu.VMEM((GROUP, *stat), f32)]
        scratch += [flags, flags] + Scatter.scratch(2, d, 2 * HEAD, 2)
        comm = {"collective_id": 2, "has_side_effects": True}
    return pl.pallas_call(
        functools.partial(_attn_back, blk=blk, scale=SCALE, inner=inner), grid=(heads,),
        in_specs=[full, full, one, one, one, one, pl.BlockSpec((1, 1, t), lambda h: (h, 0, 0)), cols, cols, cols,
                  pl.BlockSpec((None, HEAD, d), lambda h: (layer, h, 0)), tab, tab] + more,
        out_specs=outs, out_shape=shapes, scratch_shapes=scratch,
        compiler_params=params(**comm), cost_estimate=cost(22 * t * d * d + 8 * t * t * d),
    )(x, dh, q, k, v, o, lse, wq, wk, wv, wo, cos, sin, *(squares or ()))


def tables(t):
    half, lane = HEAD // 2, 128
    by = THETA ** (-jnp.arange(half, dtype=f32) / half)
    high = (jnp.arange(t // lane, dtype=f32) * lane)[:, None, None] * by
    low = jnp.arange(lane, dtype=f32)[:, None] * by
    (ch, sh), (cl, sl) = lax.optimization_barrier(((jnp.cos(high), jnp.sin(high)), (jnp.cos(low), jnp.sin(low))))
    return (ch * cl - sh * sl).reshape(t, half), (sh * cl + ch * sl).reshape(t, half)


def owner(half, late, s):
    hi, lo = s // 2, s % 2
    x, y = hi + (lo - hi) * late, lo + (hi - lo) * late
    return x * 4 + y * 2 + half


def flat(g, which, cols, per, s):
    _, blocks, _, _, n, wide = g.shape
    each = wide // cols

    def at(step):
        r = step * per + s
        return owner(r // 8, r // 4 % 2, r % 4), 0, which // each, r // 4 % 2, 0, which % each

    return pl.BlockSpec((1, blocks, 1, 1, n, cols), at)


def piece(g, which, cols, index):
    each = g.shape[5] // cols

    def at(r):
        half, late, s, block = index(r)
        return owner(half, late, s), block, which // each, late, 0, which % each

    return pl.BlockSpec((1, 1, 1, 1, g.shape[4], cols), at)


def update(refs, which, at, g, factor):
    n = len(refs) // 6
    w_ref, m_ref, v_ref, w_out, m_out, v_out = (refs[kind * n + which] for kind in range(6))
    g = g.astype(f32) * factor
    m = 0.9 * m_ref[at] + 0.1 * g
    v = 0.95 * v_ref[at] + 0.05 * g * g
    w = w_ref[at].astype(f32)
    w_out[at] = (w - 0.02 * (m * lax.rsqrt(v + 1e-8) + 0.1 * w)).astype(bf16)
    m_out[at] = m
    v_out[at] = v


def _adam(sq_ref, *refs, count, per, flats, pieces, arrays, cols):
    factor = jnp.minimum(1.0, 0.5 * lax.rsqrt(jnp.sum(sq_ref[...]) / count + 1e-30))
    first, given = flats * per, flats * per + len(pieces)
    state = refs[given : given + arrays] + refs[len(refs) - arrays :]
    part = lambda i, n: slice(i * n, (i + 1) * n)
    for at, ref in enumerate(refs[:first]):
        which, s = divmod(at, per)
        _, blocks, _, _, n, _ = ref.shape
        for k in range(blocks):
            update(state, which, (part(s, n), part(k, cols)), ref[0, k, 0, 0], factor)
    for ref, (row, col) in zip(refs[first:given], pieces):
        update(state, flats, (part(row, n), part(col, cols)), ref[0, 0, 0, 0], factor)


def adam(squares, g, arrays, layer, before, count):
    n = g.shape[4]
    d = arrays[0].shape[1]
    flats = len(arrays) // 3 - 1
    cols = g.shape[2] * g.shape[5] // (flats + 1)
    tall = arrays[flats].shape[1] // (d // n)
    across = d // cols
    if tall == n:
        per = 2
        places = [(s, k) for s in range(per) for k in range(across)]
        at = lambda r, s: r * per + s
        spec = [piece(g, flats, cols, lambda r, s=s, k=k: (k // 2, k % 2, at(r, s) % 4, at(r, s) // 4)) for s, k in places]
    else:
        per = 1
        places = [(s, k) for s in range(tall // n) for k in range(across)]
        spec = [piece(g, flats, cols, lambda r, s=s, k=k: (k, r % 2, s, r // 2)) for s, k in places]
    kinds = [pl.BlockSpec((None, n * per, a.shape[2]), lambda r: (layer, r, 0)) for a in arrays[:flats]]
    kinds = (kinds + [pl.BlockSpec((None, tall * per, d), lambda r: (layer, r, 0))]) * 3
    given = [squares] + [g] * (flats * per + len(places)) + list(arrays)
    specs = [STAT] + [flat(g, which, cols, per, s) for which in range(flats) for s in range(per)] + spec + kinds
    aliases = {}
    if before is not None:
        aliases = {len(given) + i: i for i in range(len(arrays))}
        given += list(before)
        specs += [pl.BlockSpec(memory_space=pl.ANY)] * len(arrays)
    return pl.pallas_call(
        functools.partial(_adam, count=count, per=per, flats=flats, pieces=places, arrays=len(arrays), cols=cols), grid=(d // n // per,),
        in_specs=specs, out_specs=kinds, out_shape=[jax.ShapeDtypeStruct(a.shape, a.dtype) for a in arrays],
        input_output_aliases=aliases, compiler_params=params(), cost_estimate=cost(4000 * arrays[0].size), name="adam",
    )(*given)


def solution(mesh):
    def step(x, dy, *arrays):
        weights, m, v = (arrays[i : i + 7] for i in (0, 7, 14))
        wq, wk, wv, wo, wg, wu, wd = weights
        cos, sin = tables(x.shape[1])
        layers = wq.shape[0]
        h, kept = x[0], []
        for n in range(layers):
            q, k, val, o, lse, mid = heads(h, wq, wk, wv, wo, cos, sin, n)
            kept.append((h, q, k, val, o, lse, mid))
            if n < layers - 1:
                h, *saved = mlp(mid, wg, wu, wd, n)
        parts = []

        def gather(n, a, b, own):
            parts.append((n, a, b, lax.all_gather(own, "dp")))

        h, q, k, val, o, lse, mid = kept[1]
        own, square_1, dh = mlp_back(mid, dy[0], wg, wu, wd, 1)
        gather(1, 4, 7, own)
        terms, by_h = attn_back(h, dh, q, k, val, o, lse, wq, wk, wv, wo, cos, sin, 1, None)
        h, q, k, val, o, lse, mid = kept[0]
        own, more, square_0, dh = mlp_back(mid, by_h, wg, wu, wd, 0, (*saved, terms))
        gather(1, 0, 4, more.reshape(-1, 2, *more.shape[1:]))
        gather(0, 4, 7, own)
        own, total = attn_back(h, dh, q, k, val, o, lse, wq, wk, wv, wo, cos, sin, 0, (square_1, square_0))
        gather(0, 0, 4, own)
        count = sum(w.size for w in weights)
        new = {0: None, 4: None}
        for n, a, b, g in parts:
            new[a] = adam(total, g, (*weights[a:b], *m[a:b], *v[a:b]), n, new[a], count)
        return tuple(one for i in range(3) for a, size in ((0, 4), (4, 3)) for one in new[a][size * i : size * (i + 1)])

    states, all_of = P(("rep", "dp"), None, None), P(None, None, None)
    return jax.shard_map(
        step, mesh=mesh, in_specs=(states, states) + (all_of,) * 21, out_specs=(P("rep", None, None),) * 21, check_vma=False,
    )
```
